128 devices in a mesh: row: 16 (over z, y_hi, core), col: 8 (over y_lo, x).
Axes of the slice: x: 4, y: 4 (y_hi: 2, y_lo: 2; y = y_hi * 2 + y_lo), z: 4, core: 2. Of those that a mesh axis runs over, the one named last changes fastest.
Arguments:
- reflectivity: float32 [128, 512, 2048], P(('row', 'col')), may hold values from 0 to 40
- scan_hour: int32 [128], replicated, may hold values from 0 to 11, as said below
- basin_ids: int32 [512, 16], P('row', 'col'), may hold values from 0 to 1023, as said below
Outputs:
- hourly_depth: float32 [12, 512, 2048], P(None, 'row', 'col')
- basin_depth: float32 [1024, 12], P(('row', 'col'))
The draws below stay inside these ranges and needn't reach their ends.
Inputs may be any that keep to these rules, and one draw needn't show every extreme that they name: scan_hour starts at 0, never falls, rises by at most one from one scan to the next, and every hour has 1 to 12 scans. `basin_ids`: every basin is named by at least one segment, and all segments of a basin lie in one aligned block of 8 grid rows.
All inputs are finite; a program needn't handle non-finite values.
Results may differ from the reference program's by a relative error of at most 0.00021.
Values sent between devices are 32-bit elements; how exact they have to be, the bound alone decides.
A program may use at most 64 MiB of HBM per device.

```python
import math
import jax
import jax.numpy as jnp
from jax import lax

SEG = 128
BASIN_ROWS = 8
SCANS = 128
HOURS = 12
NY = 512
NX = 2048
BASINS = 1024


def draw_scan_hour(key, part):
    spare = 11
    extra = SCANS - HOURS
    slots = jax.random.permutation(jax.random.fold_in(key, 5), HOURS * spare).astype(jnp.int32)
    chosen = slots[:extra] // spare
    hour_range = jnp.arange(HOURS, dtype=jnp.int32)
    counts = 1 + jnp.sum((chosen[:, None] == hour_range[None, :]).astype(jnp.int32), axis=0)
    ends = jnp.cumsum(counts).astype(jnp.int32)
    positions = jnp.arange(SCANS, dtype=jnp.int32)
    hours = jnp.sum((ends[None, :HOURS - 1] <= positions[:, None]).astype(jnp.int32), axis=1)
    return hours.astype(jnp.int32)


def block_order(block_key):
    return jax.random.permutation(block_key, BASIN_ROWS * (NX // SEG)).astype(jnp.int32)


def draw_basin_ids(key, part):
    seg_count = NX // SEG
    block_count = NY // BASIN_ROWS
    block_cells = BASIN_ROWS * seg_count
    block_keys = jax.random.split(jax.random.fold_in(key, 3), block_count)
    ranks = jax.vmap(block_order)(block_keys).astype(jnp.int32)
    spread = jax.random.randint(jax.random.fold_in(key, 4), (block_count, block_cells), 0, seg_count).astype(jnp.int32)
    local = jnp.where(ranks < seg_count, ranks, spread).astype(jnp.int32)
    base = jnp.arange(block_count, dtype=jnp.int32)[:, None] * seg_count + local
    labels = jax.random.permutation(jax.random.fold_in(key, 7), BASINS).astype(jnp.int32)
    return labels[base].reshape(NY, seg_count).astype(jnp.int32)


def shard_levels(own_key, dims, cuts, least, top_value):
    def one(axis_at, blocks):
        heights = jax.random.uniform(jax.random.fold_in(jax.random.fold_in(own_key, 6), axis_at), (blocks,), jnp.float32, least / len(cuts), top_value / len(cuts))
        return jnp.repeat(jnp.exp(heights), dims[axis_at] // blocks).reshape((-1,) + (1,) * (len(dims) - axis_at - 1))

    loudness = one(*cuts[0])
    for cut in cuts[1:]:
        loudness = loudness * one(*cut)
    return loudness


def setup_inputs(seed: int = 0) -> dict:
    key_list = jax.random.split(jax.random.key(seed), 4)
    return {
        "reflectivity": jnp.clip(40.0 * jax.random.uniform(key_list[0], (SCANS, NY, NX), jnp.float32) ** shard_levels(key_list[0], (SCANS, NY, NX), ((0, 128),), -0.2, 0.2), 0.0, 40.0),
        "scan_hour": draw_scan_hour(jax.random.fold_in(key_list[3], 71), 0),
        "basin_ids": draw_basin_ids(jax.random.fold_in(key_list[3], 71), 0),
    }


slope_db = math.log(10.0) / 16.0
offset_zr = math.log(200.0) / 1.6


def rain_depth(reflect):
    return jnp.exp(reflect * slope_db - offset_zr) / 12.0


def reference(reflectivity, scan_hour, basin_ids):
    def accumulate(running, scan_item):
        radar_frame, hour_slot = scan_item
        return running.at[hour_slot].add(rain_depth(radar_frame)), None

    initial = jnp.zeros((HOURS, NY, NX), jnp.float32)
    hourly, unused = lax.scan(accumulate, initial, (reflectivity, scan_hour))
    segment = hourly.reshape(HOURS, NY, NX // SEG, SEG).sum(axis=3).reshape(HOURS, -1)
    flat_ids = basin_ids.reshape(-1).astype(jnp.int32)
    totals = jax.ops.segment_sum(segment.T, flat_ids, num_segments=BASINS)
    pixels = jax.ops.segment_sum(jnp.full(flat_ids.shape, float(SEG), jnp.float32), flat_ids, num_segments=BASINS)
    return hourly, totals / pixels[:, None]
```

```python
import math

import jax
import jax.numpy as jnp
from jax import lax
from jax.experimental import pallas as pl
from jax.experimental.pallas import tpu as pltpu
from jax.sharding import PartitionSpec as P

MESH = pl.DeviceIdType.MESH
SEG = 128
HOURS = 12
CHUNKS = 4
SLOTS = (4, 5)
LOW = 11
LOG2E = 1.0 / math.log(2.0)
SCALE = math.log(10.0) / 16.0 * LOG2E
SHIFT = (math.log(200.0) / 1.6 + math.log(12.0)) * LOG2E


def rain_depth(reflect):
    return jnp.exp2(reflect * SCALE - SHIFT)


def flip(value, mask):
    if mask == 0:
        return value
    if mask == 1:
        return value + 1 - 2 * (value % 2)
    if mask == 2:
        return (value + 2) % 4
    return 3 - value


def masks(parity):
    return (1, 3) if parity == 0 else (3, 1)


def device(x, y, z, c):
    return (z * 4 + (y // 2) * 2 + c, (y % 2) * 4 + x)


def kernel(
    refl, hours, ids, out, depth,
    src, got1, own_slots0, own_slots1, own_slots2, own_slots3, got2a, got2b, got2c, got2d,
    part, part_got, part_sum, part_last,
    load_sem, send1, recv1, send2, recv2, bsend1, brecv1, bsend2, brecv2,
):
    slots_of = (own_slots0, own_slots1, own_slots2, own_slots3)
    got2_of = (got2a, got2b, got2c, got2d)
    row, col = lax.axis_index("row"), lax.axis_index("col")
    z, c = row // 4, row % 2
    y, x = ((row // 2) % 2) * 2 + col // 4, col % 4

    for j in range(CHUNKS):
        m1, m2 = masks(j % 2)
        for ry1 in range(2):
            for ry2 in range(2):
                dy = flip(y, (m1 * ry1) ^ (m2 * ry2))
                for rx1 in range(2):
                    for rx2 in range(2):
                        dx = flip(x, (m1 * rx1) ^ (m2 * rx2))
                        lanes = pl.ds(pl.multiple_of(((dy % 2) * 4 + dx) * 256, 256), 256)
                        pltpu.make_async_copy(
                            refl.at[:, dy // 2, :, j, :, lanes],
                            src.at[j, ry1, rx1, pl.ds((ry2 * 2 + rx2) * 4, 4)],
                            load_sem.at[j],
                        ).start()

    barrier = pltpu.get_barrier_semaphore()
    peers = []
    for my in (0, 1, 3):
        for mx in (0, 1, 3):
            for dz in range(4):
                for dc in range(2):
                    quad_even = mx in (0, 1) and my in (0, 1)
                    quad_odd = mx in (0, 3) and my in (0, 3)
                    if not (quad_even or quad_odd) or (dc and dz):
                        continue
                    if mx == 0 and my == 0 and dz == 0 and dc == 0:
                        continue
                    peers.append((mx, my, dz, dc))
    for mx, my, dz, dc in peers:
        core = 1 - c if dc else c
        pl.semaphore_signal(
            barrier, inc=1, device_id=device(flip(x, mx), flip(y, my), (z + dz) % 4, core), device_id_type=MESH
        )

    for j in range(CHUNKS):
        empty = jnp.zeros((8, 256), jnp.float32)
        buf, slots = got2_of[j], SLOTS[j % 2]

        @pl.loop(0, 16)
        def _(s):
            for k in range(HOURS + LOW):
                if not LOW <= k < LOW + slots:
                    buf[s, k] = empty

    pl.semaphore_wait(barrier, len(peers))

    def copy1(j, ry1, rx1, tc, sc):
        m1, _ = masks(j % 2)
        return pltpu.make_async_remote_copy(
            src_ref=src.at[j, ry1, rx1, :, tc],
            dst_ref=got1.at[j, ry1, rx1, sc],
            send_sem=send1.at[j, (ry1 * 2 + rx1) * 2 + tc],
            recv_sem=recv1.at[j, (ry1 * 2 + rx1) * 2 + sc],
            device_id=device(flip(x, m1 * rx1), flip(y, m1 * ry1), z, tc),
            device_id_type=MESH,
        )

    quads = [(0, 1), (1, 0), (1, 1)]

    def step1_copies(j, mine):
        found = []
        for ry1, rx1 in quads:
            for core in range(2):
                found.append(copy1(j, ry1, rx1, core, c) if mine else copy1(j, ry1, rx1, c, core))
        found.append(copy1(j, 0, 0, 1 - c, c) if mine else copy1(j, 0, 0, c, 1 - c))
        return found

    for j in range(CHUNKS):
        pltpu.make_async_copy(src.at[j], src.at[j], load_sem.at[j]).wait()
        for copy in step1_copies(j, True):
            copy.start()

    def base_scan(j, yy, zz):
        return zz * 32 + (yy // 2) * 16 if j % 2 == 0 else zz * 32

    def reduce1(j):
        m1, _ = masks(j % 2)
        slots = SLOTS[j % 2]
        first = hours[base_scan(j, y, z)]
        weights = []
        for ry1 in range(2):
            for rx1 in range(2):
                for core in range(2):
                    yy, xx = flip(y, m1 * ry1), flip(x, m1 * rx1)
                    cc = core if ry1 + rx1 else (c if core == 0 else 1 - c)
                    hour = hours[z * 32 + (yy // 2) * 16 + cc * 8 + (yy % 2) * 4 + xx]
                    weights.append([jnp.where(hour - first == k, 1.0, 0.0).astype(jnp.float32) for k in range(slots)])

        @pl.loop(0, 16)
        def _(t):
            total = [None] * slots
            n = 0
            for ry1 in range(2):
                for rx1 in range(2):
                    for core in range(2):
                        if ry1 + rx1:
                            raw = got1[j, ry1, rx1, core, t]
                        elif core == 0:
                            raw = src[j, 0, 0, t, c]
                        else:
                            raw = got1[j, 0, 0, 1 - c, t]
                        value = rain_depth(raw)
                        for k in range(slots):
                            term = value * weights[n][k]
                            total[k] = term if total[k] is None else total[k] + term
                        n += 1
            for k in range(slots):
                slots_of[j][t, k] = total[k]

    def copy2(j, q, dz, mine):
        _, m2 = masks(j % 2)
        ry2, rx2 = q // 2, q % 2
        slots = SLOTS[j % 2]
        target_z = (z + dz) % 4
        return pltpu.make_async_remote_copy(
            src_ref=slots_of[j].at[q * 4 + target_z],
            dst_ref=got2_of[j].at[q * 4 + dz, pl.ds(LOW, slots)],
            send_sem=send2.at[j, q * 4 + dz],
            recv_sem=recv2.at[j, q * 4 + dz],
            device_id=device(flip(x, m2 * rx2), flip(y, m2 * ry2), target_z, c),
            device_id_type=MESH,
        )

    far = [(q, dz) for q in range(4) for dz in range(4) if q or dz]

    def combine2(j):
        _, m2 = masks(j % 2)
        starts = []
        for q in range(4):
            for dz in range(4):
                yy = flip(y, m2 * (q // 2))
                starts.append(LOW - hours[base_scan(j, yy, (z - dz + 4) % 4)])
        for h in range(HOURS):
            terms = [got2_of[j][s, starts[s] + h] for s in range(16)]
            while len(terms) > 1:
                terms = [a + b for a, b in zip(terms[::2], terms[1::2])]
            out[h, j * 8 : (j + 1) * 8, :] = terms[0]

    for j in range(CHUNKS):
        for copy in step1_copies(j, False):
            copy.wait_recv()
        reduce1(j)
        for q, dz in far:
            copy2(j, q, dz, True).start()
        for k in range(SLOTS[j % 2]):
            got2_of[j][0, LOW + k] = slots_of[j][z, k]
    for j in range(CHUNKS):
        for q, dz in far:
            copy2(j, q, dz, True).wait_recv()
        combine2(j)

    tile_rows = out.shape[1]
    lane = lax.broadcasted_iota(jnp.int32, (tile_rows, 128), 1)
    owner_lane = lane
    oz, orx2, ory2 = owner_lane % 4, (owner_lane // 4) % 2, (owner_lane // 8) % 2
    oc, orx1, ory1 = (owner_lane // 16) % 2, (owner_lane // 32) % 2, owner_lane // 64

    def flip_lanes(value, bit, mask):
        return jnp.where(bit == 1, flip(value, mask), value)

    ox = flip_lanes(flip_lanes(jnp.full_like(lane, x), orx1, 1), orx2, 3)
    oy = flip_lanes(flip_lanes(jnp.full_like(lane, y), ory1, 1), ory2, 3)
    owner = (oz * 4 + (oy // 2) * 2 + oc) * 8 + (oy % 2) * 4 + ox
    share = jnp.zeros((128, 128), jnp.float32)
    for g in range(2):
        value = jnp.where(lane % 16 == HOURS, float(SEG), 0.0)
        for h in range(HOURS):
            total = jnp.sum(out[h, :, g * 128 : (g + 1) * 128], axis=1, keepdims=True)
            value = jnp.where(lane % 16 == h, total, value)
        names = ids[:, g : g + 1]
        value = jnp.where(lane // 16 == names % 8, value, 0.0)
        chosen = jnp.where(owner == names // 8, 1.0, 0.0)
        share = share + lax.dot_general(
            chosen, value, (((0,), (0,)), ((), ())),
            precision=lax.Precision.HIGHEST, preferred_element_type=jnp.float32,
        )
    part[...] = share.reshape(8, 16, 128)

    def bcopy1(ry1, rx1, tc, sc):
        return pltpu.make_async_remote_copy(
            src_ref=part.at[(ry1 * 2 + rx1) * 2 + tc],
            dst_ref=part_got.at[(ry1 * 2 + rx1) * 2 + sc],
            send_sem=bsend1.at[(ry1 * 2 + rx1) * 2 + tc],
            recv_sem=brecv1.at[(ry1 * 2 + rx1) * 2 + sc],
            device_id=device(flip(x, rx1), flip(y, ry1), z, tc),
            device_id_type=MESH,
        )

    for ry1, rx1 in quads:
        for core in range(2):
            bcopy1(ry1, rx1, core, c).start()
    bcopy1(0, 0, 1 - c, c).start()
    summed = part[c]
    for ry1, rx1 in quads:
        for core in range(2):
            bcopy1(ry1, rx1, c, core).wait_recv()
            summed = summed + part_got[(ry1 * 2 + rx1) * 2 + core]
    bcopy1(0, 0, c, 1 - c).wait_recv()
    summed = summed + part_got[1 - c]
    part_sum[...] = summed.reshape(2, 8, 128)

    def bcopy2(q, dz):
        target_z = (z + dz) % 4
        return pltpu.make_async_remote_copy(
            src_ref=part_sum.at[q // 2],
            dst_ref=part_last.at[q * 4 + dz],
            send_sem=bsend2.at[q * 4 + dz],
            recv_sem=brecv2.at[q * 4 + dz],
            device_id=device(flip(x, 3 * (q % 2)), flip(y, 3 * (q // 2)), target_z, c),
            device_id_type=MESH,
        )

    for q, dz in far:
        bcopy2(q, dz).start()
    final = part_sum[0, pl.ds(z, 1), :]
    for q, dz in far:
        bcopy2(q, dz).wait_recv()
        final = final + part_last[q * 4 + dz, pl.ds((q % 2) * 4 + z, 1), :]

    lane8 = lax.broadcasted_iota(jnp.int32, (8, 128), 1)
    row8 = lax.broadcasted_iota(jnp.int32, (8, 128), 0)
    spread = jnp.where(lane8 // 16 == row8, jnp.broadcast_to(final, (8, 128)), 0.0)
    lane_in = lax.broadcasted_iota(jnp.int32, (128, 128), 0)
    lane_out = lax.broadcasted_iota(jnp.int32, (128, 128), 1)
    pick = jnp.where(lane_in % 16 == lane_out, 1.0, 0.0)
    table = jnp.dot(spread, pick, precision=lax.Precision.HIGHEST, preferred_element_type=jnp.float32)
    depth[...] = (table / table[:, HOURS : HOURS + 1])[:, :HOURS]

    for j in range(CHUNKS):
        for copy in step1_copies(j, True):
            copy.wait_send()
        for q, dz in far:
            copy2(j, q, dz, True).wait_send()
    for ry1, rx1 in quads:
        for core in range(2):
            bcopy1(ry1, rx1, core, c).wait_send()
    bcopy1(0, 0, 1 - c, c).wait_send()
    for q, dz in far:
        bcopy2(q, dz).wait_send()


def body(reflectivity, scan_hour, basin_ids):
    vmem = pltpu.VMEM
    bands = [vmem((16, SLOTS[j % 2], 8, 256), jnp.float32) for j in range(CHUNKS)]
    padded = [vmem((16, HOURS + LOW, 8, 256), jnp.float32) for j in range(CHUNKS)]
    dma = pltpu.SemaphoreType.DMA
    return pl.pallas_call(
        kernel,
        out_shape=(
            jax.ShapeDtypeStruct((HOURS, 32, 256), jnp.float32),
            jax.ShapeDtypeStruct((8, HOURS), jnp.float32),
        ),
        in_specs=[
            pl.BlockSpec(memory_space=pl.ANY),
            pl.BlockSpec(memory_space=pltpu.SMEM),
            pl.BlockSpec(memory_space=pltpu.VMEM),
        ],
        out_specs=(pl.BlockSpec(memory_space=pltpu.VMEM), pl.BlockSpec(memory_space=pltpu.VMEM)),
        scratch_shapes=[
            vmem((CHUNKS, 2, 2, 16, 2, 8, 256), jnp.float32),
            vmem((CHUNKS, 2, 2, 2, 16, 8, 256), jnp.float32),
            *bands,
            *padded,
            vmem((8, 16, 128), jnp.float32),
            vmem((8, 16, 128), jnp.float32),
            vmem((2, 8, 128), jnp.float32),
            vmem((16, 8, 128), jnp.float32),
            dma((CHUNKS,)),
            dma((CHUNKS, 8)),
            dma((CHUNKS, 8)),
            dma((CHUNKS, 16)),
            dma((CHUNKS, 16)),
            dma((8,)),
            dma((8,)),
            dma((16,)),
            dma((16,)),
        ],
        compiler_params=pltpu.CompilerParams(collective_id=0, has_side_effects=True, vmem_limit_bytes=56 * 1024 * 1024),
    )(reflectivity.reshape(4, 2, 2, 4, 8, 2048), scan_hour, basin_ids)


def solution(mesh):
    placed = (P(("row", "col"), None, None), P(), P("row", "col"))
    return jax.shard_map(
        body,
        mesh=mesh,
        in_specs=placed,
        out_specs=(P(None, "row", "col"), P(("row", "col"), None)),
        check_vma=False,
    )
```

```python
import math

import jax
import jax.numpy as jnp
from jax import lax
from jax.experimental import pallas as pl
from jax.experimental.pallas import tpu as pltpu
from jax.sharding import PartitionSpec as P

MESH = pl.DeviceIdType.MESH
SEG = 128
HOURS = 12
BANDS = 4
CHUNKS = 8
SLOTS = (4, 5)
LOW = 11
LOG2E = 1.0 / math.log(2.0)
SCALE = math.log(10.0) / 16.0 * LOG2E
SHIFT = (math.log(200.0) / 1.6 + math.log(12.0)) * LOG2E


def rain_depth(reflect):
    return jnp.exp2(reflect * SCALE - SHIFT)


def flip(value, mask):
    if mask == 0:
        return value
    if mask == 1:
        return value + 1 - 2 * (value % 2)
    if mask == 2:
        return (value + 2) % 4
    return 3 - value


def masks(parity):
    return (1, 3) if parity == 0 else (3, 1)


def device(x, y, z, c):
    return (z * 4 + (y // 2) * 2 + c, (y % 2) * 4 + x)


def kernel(refl, hours, ids, out, table_out, *scratch):
    src, got1 = scratch[:2]
    slots_of, gotz, sumz, gotq = (scratch[2 + CHUNKS * i : 2 + CHUNKS * (i + 1)] for i in range(4))
    (
        part, part_got, part_sum, part_last,
        load_sem, send1, recv1, sendz, recvz, sendq, recvq, bsend1, brecv1, bsend2, brecv2, bsend3, brecv3,
    ) = scratch[2 + CHUNKS * 4 :]
    row, col = lax.axis_index("row"), lax.axis_index("col")
    z, c = row // 4, row % 2
    y, x = ((row // 2) % 2) * 2 + col // 4, col % 4

    for ch in range(CHUNKS):
        m1, m2 = masks(ch % 2)
        for ry1 in range(2):
            for rx1 in range(2):
                for q in range(4):
                    dy = flip(y, (m1 * ry1) ^ (m2 * (q // 2)))
                    dx = flip(x, (m1 * rx1) ^ (m2 * (q % 2)))
                    lanes = pl.ds(pl.multiple_of(((dy % 2) * 4 + dx) * 256 + (ch % 2) * 128, 128), 128)
                    pltpu.make_async_copy(
                        refl.at[:, dy // 2, :, ch // 2, :, lanes],
                        src.at[ch, ry1, rx1, :, q],
                        load_sem.at[ch],
                    ).start()

    barrier = pltpu.get_barrier_semaphore()
    quads = [(0, 1), (1, 0), (1, 1)]
    peers = [device(x, y, z, 1 - c)]
    for mask in (1, 3):
        for ry, rx in quads:
            for core in range(2):
                peers.append(device(flip(x, mask * rx), flip(y, mask * ry), z, core))
    for dz in (1, 2, 3):
        peers.append(device(x, y, (z + dz) % 4, c))
    for peer in peers:
        pl.semaphore_signal(barrier, inc=1, device_id=peer, device_id_type=MESH)

    for ch in range(CHUNKS):
        empty = jnp.zeros((4, 8, 128), jnp.float32)
        buf, slots = gotz[ch], SLOTS[ch % 2]

        @pl.loop(0, 4)
        def _(s):
            for k in range(HOURS + LOW):
                if not LOW <= k < LOW + slots:
                    buf[s, k] = empty

    pl.semaphore_wait(barrier, len(peers))

    def copy1(ch, ry1, rx1, tc, sc):
        m1, _ = masks(ch % 2)
        return pltpu.make_async_remote_copy(
            src_ref=src.at[ch, ry1, rx1, :, :, tc],
            dst_ref=got1.at[ch, ry1, rx1, sc],
            send_sem=send1.at[ch, (ry1 * 2 + rx1) * 2 + tc],
            recv_sem=recv1.at[ch, (ry1 * 2 + rx1) * 2 + sc],
            device_id=device(flip(x, m1 * rx1), flip(y, m1 * ry1), z, tc),
            device_id_type=MESH,
        )

    def step1_copies(ch, mine):
        found = []
        for ry1, rx1 in quads:
            for core in range(2):
                found.append(copy1(ch, ry1, rx1, core, c) if mine else copy1(ch, ry1, rx1, c, core))
        found.append(copy1(ch, 0, 0, 1 - c, c) if mine else copy1(ch, 0, 0, c, 1 - c))
        return found

    def base_scan(ch, zz):
        return zz * 32 + (y // 2) * 16 if ch % 2 == 0 else zz * 32

    def reduce1(ch):
        m1, _ = masks(ch % 2)
        slots = SLOTS[ch % 2]
        first = hours[base_scan(ch, z)]
        weights = []
        for ry1 in range(2):
            for rx1 in range(2):
                for core in range(2):
                    yy, xx = flip(y, m1 * ry1), flip(x, m1 * rx1)
                    cc = core if ry1 + rx1 else (c if core == 0 else 1 - c)
                    hour = hours[z * 32 + (yy // 2) * 16 + cc * 8 + (yy % 2) * 4 + xx]
                    weights.append([jnp.where(hour - first == k, 1.0, 0.0).astype(jnp.float32) for k in range(slots)])

        @pl.loop(0, 4)
        def _(zt):
            for part_q in (0, 2):
                pair = pl.ds(part_q, 2)
                total = [None] * slots
                n = 0
                for ry1 in range(2):
                    for rx1 in range(2):
                        for core in range(2):
                            if ry1 + rx1:
                                raw = got1[ch, ry1, rx1, core, zt, pair]
                            elif core == 0:
                                raw = src[ch, 0, 0, zt, pair, c]
                            else:
                                raw = got1[ch, 0, 0, 1 - c, zt, pair]
                            value = rain_depth(raw)
                            for k in range(slots):
                                term = value * weights[n][k]
                                total[k] = term if total[k] is None else total[k] + term
                            n += 1
                for k in range(slots):
                    slots_of[ch][zt, k, pair] = total[k]

    def copyz(ch, dz):
        target_z = (z + dz) % 4
        return pltpu.make_async_remote_copy(
            src_ref=slots_of[ch].at[target_z],
            dst_ref=gotz[ch].at[dz, pl.ds(LOW, SLOTS[ch % 2])],
            send_sem=sendz.at[ch, dz],
            recv_sem=recvz.at[ch, dz],
            device_id=device(x, y, target_z, c),
            device_id_type=MESH,
        )

    def combinez(ch):
        starts = [LOW - hours[base_scan(ch, (z - dz + 4) % 4)] for dz in range(4)]
        for h in range(HOURS):
            terms = [gotz[ch][dz, starts[dz] + h] for dz in range(4)]
            sumz[ch][:, h] = (terms[0] + terms[1]) + (terms[2] + terms[3])

    def copyq(ch, q):
        _, m2 = masks(ch % 2)
        return pltpu.make_async_remote_copy(
            src_ref=sumz[ch].at[q],
            dst_ref=gotq[ch].at[q - 1],
            send_sem=sendq.at[ch, q],
            recv_sem=recvq.at[ch, q],
            device_id=device(flip(x, m2 * (q % 2)), flip(y, m2 * (q // 2)), z, c),
            device_id_type=MESH,
        )

    for ch in range(CHUNKS):
        pltpu.make_async_copy(src.at[ch], src.at[ch], load_sem.at[ch]).wait()
        for copy in step1_copies(ch, True):
            copy.start()

    def first(pair):
        for ch in (2 * pair, 2 * pair + 1):
            for copy in step1_copies(ch, False):
                copy.wait_recv()
            reduce1(ch)
            for dz in (2, 1, 3):
                copyz(ch, dz).start()
            for k in range(SLOTS[ch % 2]):
                gotz[ch][0, LOW + k] = slots_of[ch][z, k]

    def second(pair):
        for ch in (2 * pair, 2 * pair + 1):
            for dz in (1, 2, 3):
                copyz(ch, dz).wait_recv()
            combinez(ch)
            for q in (3, 1, 2):
                copyq(ch, q).start()

    def third(pair):
        for ch in (2 * pair, 2 * pair + 1):
            for q in (1, 2, 3):
                copyq(ch, q).wait_recv()
            j, half = ch // 2, ch % 2
            for h in range(HOURS):
                out[h, j * 8 : (j + 1) * 8, half * 128 : (half + 1) * 128] = (
                    (sumz[ch][0, h] + gotq[ch][0, h]) + (gotq[ch][1, h] + gotq[ch][2, h])
                )

    for pair in range(BANDS + 2):
        if pair < BANDS:
            first(pair)
        if 1 <= pair <= BANDS:
            second(pair - 1)
        if pair >= 2:
            third(pair - 2)

    tile_rows = out.shape[1]
    lane = lax.broadcasted_iota(jnp.int32, (tile_rows, 128), 1)
    rank = lax.broadcasted_iota(jnp.int32, (128, tile_rows), 0)
    oz, orx2, ory2 = rank % 4, (rank // 4) % 2, (rank // 8) % 2
    oc, orx1, ory1 = (rank // 16) % 2, (rank // 32) % 2, rank // 64

    def flip_each(value, bit, mask):
        return jnp.where(bit == 1, flip(value, mask), value)

    ox = flip_each(flip_each(jnp.full_like(rank, x), orx1, 1), orx2, 3)
    oy = flip_each(flip_each(jnp.full_like(rank, y), ory1, 1), ory2, 3)
    owner = (oz * 4 + (oy // 2) * 2 + oc) * 8 + (oy % 2) * 4 + ox
    square = (tile_rows, tile_rows)
    diagonal = lax.broadcasted_iota(jnp.int32, square, 0) == lax.broadcasted_iota(jnp.int32, square, 1)
    share = jnp.zeros((128, 128), jnp.float32)
    for g in range(2):
        value = jnp.where(lane % 16 == HOURS, float(SEG), 0.0)
        for h in range(HOURS):
            total = jnp.sum(out[h, :, g * 128 : (g + 1) * 128], axis=1, keepdims=True)
            value = jnp.where(lane % 16 == h, total, value)
        names = ids[g : g + 1, :]
        place = (names % 8).astype(jnp.float32)
        place = jnp.sum(jnp.where(diagonal, place, 0.0), axis=1, keepdims=True)
        value = jnp.where((lane // 16).astype(jnp.float32) == place, value, 0.0)
        chosen = jnp.where(owner == names // 8, 1.0, 0.0)
        share = share + jnp.dot(
            chosen, value, precision=lax.Precision.HIGHEST, preferred_element_type=jnp.float32
        )
    part[...] = share.reshape(8, 16, 128)

    def bcopy1(ry1, rx1, tc, sc):
        return pltpu.make_async_remote_copy(
            src_ref=part.at[(ry1 * 2 + rx1) * 2 + tc],
            dst_ref=part_got.at[(ry1 * 2 + rx1) * 2 + sc],
            send_sem=bsend1.at[(ry1 * 2 + rx1) * 2 + tc],
            recv_sem=brecv1.at[(ry1 * 2 + rx1) * 2 + sc],
            device_id=device(flip(x, rx1), flip(y, ry1), z, tc),
            device_id_type=MESH,
        )

    for ry1, rx1 in quads:
        for core in range(2):
            bcopy1(ry1, rx1, core, c).start()
    bcopy1(0, 0, 1 - c, c).start()
    summed = part[c]
    for ry1, rx1 in quads:
        for core in range(2):
            bcopy1(ry1, rx1, c, core).wait_recv()
            summed = summed + part_got[(ry1 * 2 + rx1) * 2 + core]
    bcopy1(0, 0, c, 1 - c).wait_recv()
    summed = summed + part_got[1 - c]
    part_sum[0] = summed

    def bcopy2(dz):
        return pltpu.make_async_remote_copy(
            src_ref=part_sum.at[0],
            dst_ref=part_last.at[dz],
            send_sem=bsend2.at[dz],
            recv_sem=brecv2.at[dz],
            device_id=device(x, y, (z + dz) % 4, c),
            device_id_type=MESH,
        )

    def bcopy3(q):
        return pltpu.make_async_remote_copy(
            src_ref=part_sum.at[1],
            dst_ref=part_last.at[3 + q],
            send_sem=bsend3.at[q],
            recv_sem=brecv3.at[q],
            device_id=device(flip(x, 3 * (q % 2)), flip(y, 3 * (q // 2)), z, c),
            device_id_type=MESH,
        )

    for dz in (1, 2, 3):
        bcopy2(dz).start()
    for dz in (1, 2, 3):
        bcopy2(dz).wait_recv()
        summed = summed + part_last[dz]
    part_sum[1] = summed
    for q in (1, 2, 3):
        bcopy3(q).start()
    final = part_sum[1, pl.ds(z, 1), :]
    for q in (1, 2, 3):
        bcopy3(q).wait_recv()
        final = final + part_last[3 + q, pl.ds(q * 4 + z, 1), :]

    lane8 = lax.broadcasted_iota(jnp.int32, (8, 128), 1)
    row8 = lax.broadcasted_iota(jnp.int32, (8, 128), 0)
    spread = jnp.where(lane8 // 16 == row8, jnp.broadcast_to(final, (8, 128)), 0.0)
    lane_in = lax.broadcasted_iota(jnp.int32, (128, 128), 0)
    lane_out = lax.broadcasted_iota(jnp.int32, (128, 128), 1)
    pick = jnp.where(lane_in % 16 == lane_out, 1.0, 0.0)
    table_out[...] = jnp.dot(spread, pick, precision=lax.Precision.HIGHEST, preferred_element_type=jnp.float32)

    for ch in range(CHUNKS):
        for copy in step1_copies(ch, True):
            copy.wait_send()
        for dz in (1, 2, 3):
            copyz(ch, dz).wait_send()
        for q in (1, 2, 3):
            copyq(ch, q).wait_send()
    for ry1, rx1 in quads:
        for core in range(2):
            bcopy1(ry1, rx1, core, c).wait_send()
    bcopy1(0, 0, 1 - c, c).wait_send()
    for n in (1, 2, 3):
        bcopy2(n).wait_send()
        bcopy3(n).wait_send()


def finish(hourly, table, out, depth):
    out[...] = hourly[...]
    depth[...] = (table[...] / table[:, HOURS : HOURS + 1])[:, :HOURS]


def body(reflectivity, scan_hour, basin_ids):
    def vmem(*shape):
        return pltpu.VMEM(shape, jnp.float32)

    def dma(*shape):
        return pltpu.SemaphoreType.DMA(shape)

    chunks = range(CHUNKS)
    scratch = [
        vmem(CHUNKS, 2, 2, 4, 4, 2, 8, 128),
        vmem(CHUNKS, 2, 2, 2, 4, 4, 8, 128),
        *[vmem(4, SLOTS[ch % 2], 4, 8, 128) for ch in chunks],
        *[vmem(4, HOURS + LOW, 4, 8, 128) for ch in chunks],
        *[vmem(4, HOURS, 8, 128) for ch in chunks],
        *[vmem(3, HOURS, 8, 128) for ch in chunks],
        vmem(8, 16, 128), vmem(8, 16, 128), vmem(2, 16, 128), vmem(7, 16, 128),
        dma(CHUNKS), dma(CHUNKS, 8), dma(CHUNKS, 8), dma(CHUNKS, 4), dma(CHUNKS, 4), dma(CHUNKS, 4), dma(CHUNKS, 4),
        dma(8), dma(8), dma(4), dma(4), dma(4), dma(4),
    ]
    block = pl.BlockSpec(memory_space=pltpu.VMEM)
    hourly, table = pl.pallas_call(
        kernel,
        out_shape=(
            jax.ShapeDtypeStruct((HOURS, 32, 256), jnp.float32),
            jax.ShapeDtypeStruct((8, 128), jnp.float32),
        ),
        in_specs=[pl.BlockSpec(memory_space=pl.ANY), pl.BlockSpec(memory_space=pltpu.SMEM), block],
        out_specs=(block, block),
        scratch_shapes=scratch,
        compiler_params=pltpu.CompilerParams(
            collective_id=0, has_side_effects=True, vmem_limit_bytes=52 * 1024 * 1024
        ),
    )(reflectivity.reshape(4, 2, 2, BANDS, 8, 2048), scan_hour, basin_ids.T)
    return pl.pallas_call(
        finish,
        out_shape=(
            jax.ShapeDtypeStruct((HOURS, 32, 256), jnp.float32),
            jax.ShapeDtypeStruct((8, HOURS), jnp.float32),
        ),
        in_specs=[block, block],
        out_specs=(block, block),
        compiler_params=pltpu.CompilerParams(vmem_limit_bytes=8 * 1024 * 1024),
    )(hourly, table)


def solution(mesh):
    placed = (P(("row", "col"), None, None), P(), P("row", "col"))
    return jax.shard_map(
        body,
        mesh=mesh,
        in_specs=placed,
        out_specs=(P(None, "row", "col"), P(("row", "col"), None)),
        check_vma=False,
    )
```

```python
import math

import jax
import jax.numpy as jnp
from jax import lax
from jax.experimental import pallas as pl
from jax.experimental.pallas import tpu as pltpu
from jax.sharding import PartitionSpec as P

MESH = pl.DeviceIdType.MESH
SEG = 128
HOURS = 12
BANDS = 4
CHUNKS = 8
SLOTS = (4, 5)
LOW = 11
LOG2E = 1.0 / math.log(2.0)
SCALE = math.log(10.0) / 16.0 * LOG2E
SHIFT = (math.log(200.0) / 1.6 + math.log(12.0)) * LOG2E


def rain_depth(reflect):
    return jnp.exp2(reflect * SCALE - SHIFT)


def flip(value, mask):
    if mask == 0:
        return value
    if mask == 1:
        return value + 1 - 2 * (value % 2)
    if mask == 2:
        return (value + 2) % 4
    return 3 - value


def masks(parity):
    return (1, 3) if parity == 0 else (3, 1)


def device(x, y, z, c):
    return (z * 4 + (y // 2) * 2 + c, (y % 2) * 4 + x)


def kernel(refl, hours, ids, out, table_out, *scratch):
    src, got1 = scratch[:2]
    slots_of, gotz, sumz, gotq = (scratch[2 + CHUNKS * i : 2 + CHUNKS * (i + 1)] for i in range(4))
    (
        own_seg, got_seg, seg_hours, got_hours, seg_pack, got_pack, part, part_got, part_sum, part_last, row_sum, row_got,
        load_sem, send1, recv1, sendz, recvz, sendq, recvq, esend1, erecv1, esend2, erecv2, esend3, erecv3,
        bsend1, brecv1, bsend2, brecv2, bsend3, brecv3,
    ) = scratch[2 + CHUNKS * 4 :]
    row, col = lax.axis_index("row"), lax.axis_index("col")
    z, c = row // 4, row % 2
    y, x = ((row // 2) % 2) * 2 + col // 4, col % 4

    for ch in range(CHUNKS):
        m1, m2 = masks(ch % 2)
        for ry1 in range(2):
            for rx1 in range(2):
                for q in range(4):
                    dy = flip(y, (m1 * ry1) ^ (m2 * (q // 2)))
                    dx = flip(x, (m1 * rx1) ^ (m2 * (q % 2)))
                    lanes = pl.ds(pl.multiple_of(((dy % 2) * 4 + dx) * 256 + (ch % 2) * 128, 128), 128)
                    pltpu.make_async_copy(
                        refl.at[:, dy // 2, :, ch // 2, :, lanes],
                        src.at[ch, ry1, rx1, :, q],
                        load_sem.at[ch],
                    ).start()

    barrier = pltpu.get_barrier_semaphore()
    quads = [(0, 1), (1, 0), (1, 1)]
    peers = [device(x, y, z, 1 - c)]
    for mask in (1, 3):
        for ry, rx in quads:
            for core in range(2):
                peers.append(device(flip(x, mask * rx), flip(y, mask * ry), z, core))
    for dz in (1, 2, 3):
        peers.append(device(x, y, (z + dz) % 4, c))
    for peer in peers:
        pl.semaphore_signal(barrier, inc=1, device_id=peer, device_id_type=MESH)

    for ch in range(CHUNKS):
        empty = jnp.zeros((4, 8, 128), jnp.float32)
        buf, slots = gotz[ch], SLOTS[ch % 2]

        @pl.loop(0, 4)
        def _(s):
            for k in range(HOURS + LOW):
                if not LOW <= k < LOW + slots:
                    buf[s, k] = empty

    pl.semaphore_wait(barrier, len(peers))

    def copy1(ch, ry1, rx1, tc, sc):
        m1, _ = masks(ch % 2)
        return pltpu.make_async_remote_copy(
            src_ref=src.at[ch, ry1, rx1, :, :, tc],
            dst_ref=got1.at[ch, ry1, rx1, sc],
            send_sem=send1.at[ch, (ry1 * 2 + rx1) * 2 + tc],
            recv_sem=recv1.at[ch, (ry1 * 2 + rx1) * 2 + sc],
            device_id=device(flip(x, m1 * rx1), flip(y, m1 * ry1), z, tc),
            device_id_type=MESH,
        )

    def step1_copies(ch, mine):
        found = []
        for ry1, rx1 in quads:
            for core in range(2):
                found.append(copy1(ch, ry1, rx1, core, c) if mine else copy1(ch, ry1, rx1, c, core))
        found.append(copy1(ch, 0, 0, 1 - c, c) if mine else copy1(ch, 0, 0, c, 1 - c))
        return found

    def base_scan(ch, zz):
        return zz * 32 + (y // 2) * 16 if ch % 2 == 0 else zz * 32

    def reduce1(ch):
        m1, _ = masks(ch % 2)
        slots = SLOTS[ch % 2]
        first = hours[base_scan(ch, z)]
        weights = []
        for ry1 in range(2):
            for rx1 in range(2):
                for core in range(2):
                    yy, xx = flip(y, m1 * ry1), flip(x, m1 * rx1)
                    cc = core if ry1 + rx1 else (c if core == 0 else 1 - c)
                    hour = hours[z * 32 + (yy // 2) * 16 + cc * 8 + (yy % 2) * 4 + xx]
                    weights.append([jnp.where(hour - first == k, 1.0, 0.0).astype(jnp.float32) for k in range(slots)])

        @pl.loop(0, 4)
        def _(zt):
            for part_q in (0, 2):
                pair = pl.ds(part_q, 2)
                total = [None] * slots
                n = 0
                for ry1 in range(2):
                    for rx1 in range(2):
                        for core in range(2):
                            if ry1 + rx1:
                                raw = got1[ch, ry1, rx1, core, zt, pair]
                            elif core == 0:
                                raw = src[ch, 0, 0, zt, pair, c]
                            else:
                                raw = got1[ch, 0, 0, 1 - c, zt, pair]
                            value = rain_depth(raw)
                            for k in range(slots):
                                term = value * weights[n][k]
                                total[k] = term if total[k] is None else total[k] + term
                            n += 1
                for k in range(slots):
                    slots_of[ch][zt, k, pair] = total[k]

    def copyz(ch, dz):
        target_z = (z + dz) % 4
        return pltpu.make_async_remote_copy(
            src_ref=slots_of[ch].at[target_z],
            dst_ref=gotz[ch].at[dz, pl.ds(LOW, SLOTS[ch % 2])],
            send_sem=sendz.at[ch, dz],
            recv_sem=recvz.at[ch, dz],
            device_id=device(x, y, target_z, c),
            device_id_type=MESH,
        )

    def combinez(ch):
        starts = [LOW - hours[base_scan(ch, (z - dz + 4) % 4)] for dz in range(4)]
        for h in range(HOURS):
            terms = [gotz[ch][dz, starts[dz] + h] for dz in range(4)]
            sumz[ch][:, h] = (terms[0] + terms[1]) + (terms[2] + terms[3])

    def copyq(ch, q):
        _, m2 = masks(ch % 2)
        return pltpu.make_async_remote_copy(
            src_ref=sumz[ch].at[q],
            dst_ref=gotq[ch].at[q - 1],
            send_sem=sendq.at[ch, q],
            recv_sem=recvq.at[ch, q],
            device_id=device(flip(x, m2 * (q % 2)), flip(y, m2 * (q // 2)), z, c),
            device_id_type=MESH,
        )

    def loaded(*which):
        for ch in which:
            pltpu.make_async_copy(src.at[ch], src.at[ch], load_sem.at[ch]).wait()

    def start1(pair):
        for one, two in zip(step1_copies(2 * pair, True), step1_copies(2 * pair + 1, True)):
            one.start()
            two.start()

    def first(pair):
        for ch in (2 * pair, 2 * pair + 1):
            for copy in step1_copies(ch, False):
                copy.wait_recv()
            reduce1(ch)
            for dz in (2, 1, 3):
                copyz(ch, dz).start()
            for k in range(SLOTS[ch % 2]):
                gotz[ch][0, LOW + k] = slots_of[ch][z, k]

    def second(pair):
        for ch in (2 * pair, 2 * pair + 1):
            for dz in (1, 2, 3):
                copyz(ch, dz).wait_recv()
            combinez(ch)
            for q in (3, 1, 2):
                copyq(ch, q).start()

    def third(pair):
        for ch in (2 * pair, 2 * pair + 1):
            for q in (1, 2, 3):
                copyq(ch, q).wait_recv()
            j, half = ch // 2, ch % 2
            for h in range(HOURS):
                out[h, j * 8 : (j + 1) * 8, half * 128 : (half + 1) * 128] = (
                    (sumz[ch][0, h] + gotq[ch][0, h]) + (gotq[ch][1, h] + gotq[ch][2, h])
                )

    lane = lax.broadcasted_iota(jnp.int32, (8, 128), 1)

    def own_segments():
        def one_z(zt, totals):
            totals = list(totals)
            here = lane - zt * 32
            for q in range(4):
                for ch in range(CHUNKS):
                    spot = here == q * 8 + ch
                    for n in range(8):
                        ey1, ex1, core = n // 4, (n // 2) % 2, n % 2
                        if ch % 2 == 0:
                            raw = src[ch, ey1, ex1, zt, q, core]
                        else:
                            raw = src[ch, q // 2, q % 2, zt, ey1 * 2 + ex1, core]
                        total = jnp.sum(rain_depth(raw), axis=1, keepdims=True)
                        totals[n] = jnp.where(spot, total, totals[n])
            return tuple(totals)

        totals = lax.fori_loop(0, 4, one_z, tuple(jnp.zeros((8, 128), jnp.float32) for _ in range(8)))
        for n in range(8):
            own_seg[n // 4, (n // 2) % 2, n % 2] = totals[n]

    def ecopy1(ry1, rx1, tc, sc):
        n = (ry1 * 2 + rx1) * 2
        return pltpu.make_async_remote_copy(
            src_ref=own_seg.at[ry1, rx1, tc],
            dst_ref=got_seg.at[ry1, rx1, sc],
            send_sem=esend1.at[n + tc],
            recv_sem=erecv1.at[n + sc],
            device_id=device(flip(x, rx1), flip(y, ry1), z, tc),
            device_id_type=MESH,
        )

    def ecopy2(dz):
        return pltpu.make_async_remote_copy(
            src_ref=seg_hours,
            dst_ref=got_hours.at[dz - 1],
            send_sem=esend2.at[dz],
            recv_sem=erecv2.at[dz],
            device_id=device(x, y, (z + dz) % 4, c),
            device_id_type=MESH,
        )

    def ecopy3(q):
        return pltpu.make_async_remote_copy(
            src_ref=seg_pack,
            dst_ref=got_pack.at[q - 1],
            send_sem=esend3.at[q],
            recv_sem=erecv3.at[q],
            device_id=device(flip(x, 3 * (q % 2)), flip(y, 3 * (q // 2)), z, c),
            device_id_type=MESH,
        )

    def quad_out(copy):
        found = [copy(ry1, rx1, core, c) for ry1, rx1 in quads for core in range(2)]
        return found + [copy(0, 0, 1 - c, c)]

    def quad_in(copy):
        found = [copy(ry1, rx1, c, core) for ry1, rx1 in quads for core in range(2)]
        return found + [copy(0, 0, c, 1 - c)]

    def segments1():
        loaded(*range(2, CHUNKS))
        own_segments()
        for copy in quad_out(ecopy1):
            copy.start()

    def segments2():
        for copy in quad_in(ecopy1):
            copy.wait_recv()
        totals = [None] * HOURS
        for ry1 in range(2):
            for rx1 in range(2):
                for core in range(2):
                    yy, xx = flip(y, ry1), flip(x, rx1)
                    if ry1 + rx1:
                        cc, value = core, got_seg[ry1, rx1, core]
                    elif core == 0:
                        cc, value = c, own_seg[0, 0, c]
                    else:
                        cc, value = 1 - c, got_seg[0, 0, 1 - c]
                    hour = hours[z * 32 + (yy // 2) * 16 + cc * 8 + (yy % 2) * 4 + xx]
                    for h in range(HOURS):
                        term = value * jnp.where(hour == h, 1.0, 0.0).astype(jnp.float32)
                        totals[h] = term if totals[h] is None else totals[h] + term
        for h in range(HOURS):
            seg_hours[h] = totals[h]
        for dz in (2, 1, 3):
            ecopy2(dz).start()

    def segments3():
        for dz in (1, 2, 3):
            ecopy2(dz).wait_recv()
        for k in range(HOURS // 4):
            packed = jnp.zeros((8, 128), jnp.float32)
            for h in range(4 * k, 4 * k + 4):
                value = (seg_hours[h] + got_hours[0, h]) + (got_hours[1, h] + got_hours[2, h])
                value = jnp.where(lane // 32 == z, value, 0.0)
                value = value + pltpu.roll(value, 64, 1)
                value = value + pltpu.roll(value, 32, 1)
                packed = jnp.where(lane // 32 == h % 4, value, packed)
            seg_pack[k] = packed
        for q in (3, 1, 2):
            ecopy3(q).start()

    def shares():
        for q in (1, 2, 3):
            ecopy3(q).wait_recv()
        table = []
        for k in range(HOURS // 4):
            value = seg_pack[k]
            for q in (1, 2, 3):
                value = value + pltpu.roll(got_pack[q - 1, k], 128 - 8 * q, 1)
            table.append(value)
        tile_rows = out.shape[1]
        wide = lax.broadcasted_iota(jnp.int32, (tile_rows, 128), 1)
        rank = lax.broadcasted_iota(jnp.int32, (128, tile_rows), 0)
        oz, orx2, ory2 = rank % 4, (rank // 4) % 2, (rank // 8) % 2
        oc, orx1, ory1 = (rank // 16) % 2, (rank // 32) % 2, rank // 64

        def flip_each(value, bit, mask):
            return jnp.where(bit == 1, flip(value, mask), value)

        ox = flip_each(flip_each(jnp.full_like(rank, x), orx1, 1), orx2, 3)
        oy = flip_each(flip_each(jnp.full_like(rank, y), ory1, 1), ory2, 3)
        owner = (oz * 4 + (oy // 2) * 2 + oc) * 8 + (oy % 2) * 4 + ox
        square = (tile_rows, tile_rows)
        diagonal = lax.broadcasted_iota(jnp.int32, square, 0) == lax.broadcasted_iota(jnp.int32, square, 1)
        share = jnp.zeros((128, 128), jnp.float32)
        for g in range(2):
            bands = []
            for j in range(BANDS):
                value = jnp.where(lane % 16 == HOURS, float(SEG), 0.0)
                for h in range(HOURS):
                    at = (h % 4) * 32 + j * 2 + g
                    value = jnp.where(lane % 16 == h, table[h // 4][:, at : at + 1], value)
                bands.append(value)
            value = jnp.concatenate(bands, axis=0)
            names = ids[g : g + 1, :]
            place = (names % 8).astype(jnp.float32)
            place = jnp.sum(jnp.where(diagonal, place, 0.0), axis=1, keepdims=True)
            value = jnp.where((wide // 16).astype(jnp.float32) == place, value, 0.0)
            chosen = jnp.where(owner == names // 8, 1.0, 0.0)
            share = share + jnp.dot(
                chosen, value, precision=lax.Precision.HIGHEST, preferred_element_type=jnp.float32
            )
        part[...] = share.reshape(8, 16, 128)
        for copy in quad_out(bcopy1):
            copy.start()

    def bcopy1(ry1, rx1, tc, sc):
        n = (ry1 * 2 + rx1) * 2
        return pltpu.make_async_remote_copy(
            src_ref=part.at[n + tc],
            dst_ref=part_got.at[n + sc],
            send_sem=bsend1.at[n + tc],
            recv_sem=brecv1.at[n + sc],
            device_id=device(flip(x, rx1), flip(y, ry1), z, tc),
            device_id_type=MESH,
        )

    def bcopy2(q):
        return pltpu.make_async_remote_copy(
            src_ref=part_sum,
            dst_ref=part_last.at[q - 1],
            send_sem=bsend2.at[q],
            recv_sem=brecv2.at[q],
            device_id=device(flip(x, 3 * (q % 2)), flip(y, 3 * (q // 2)), z, c),
            device_id_type=MESH,
        )

    def bcopy3(dz):
        return pltpu.make_async_remote_copy(
            src_ref=row_sum,
            dst_ref=row_got.at[dz - 1],
            send_sem=bsend3.at[dz],
            recv_sem=brecv3.at[dz],
            device_id=device(x, y, (z + dz) % 4, c),
            device_id_type=MESH,
        )

    def shares2():
        for copy in quad_in(bcopy1):
            copy.wait_recv()
        summed = part[c] + part_got[1 - c]
        for ry1, rx1 in quads:
            for core in range(2):
                summed = summed + part_got[(ry1 * 2 + rx1) * 2 + core]
        part_sum[...] = summed
        for q in (3, 1, 2):
            bcopy2(q).start()

    def shares3():
        for q in (1, 2, 3):
            bcopy2(q).wait_recv()
        row_sum[...] = jnp.zeros((8, 128), jnp.float32)
        row_sum[0:4] = (part_sum[0:4] + part_last[0, 4:8]) + (part_last[1, 8:12] + part_last[2, 12:16])
        for dz in (2, 1, 3):
            bcopy3(dz).start()

    def shares4():
        final = row_sum[pl.ds(z, 1), :]
        for dz in (1, 2, 3):
            bcopy3(dz).wait_recv()
        for dz in (1, 2, 3):
            final = final + row_got[dz - 1, pl.ds(z, 1), :]
        row8 = lax.broadcasted_iota(jnp.int32, (8, 128), 0)
        spread = jnp.where(lane // 16 == row8, jnp.broadcast_to(final, (8, 128)), 0.0)
        lane_in = lax.broadcasted_iota(jnp.int32, (128, 128), 0)
        lane_out = lax.broadcasted_iota(jnp.int32, (128, 128), 1)
        pick = jnp.where(lane_in % 16 == lane_out, 1.0, 0.0)
        table_out[...] = jnp.dot(
            spread, pick, precision=lax.Precision.HIGHEST, preferred_element_type=jnp.float32
        )

    loaded(0, 1)
    start1(0)
    segments1()
    start1(1)
    first(0)
    segments2()
    start1(2)
    first(1)
    segments3()
    start1(3)
    second(0)
    first(2)
    shares()
    second(1)
    third(0)
    first(3)
    shares2()
    second(2)
    third(1)
    shares3()
    second(3)
    third(2)
    shares4()
    third(3)

    for ch in range(CHUNKS):
        for copy in step1_copies(ch, True):
            copy.wait_send()
        for dz in (1, 2, 3):
            copyz(ch, dz).wait_send()
        for q in (1, 2, 3):
            copyq(ch, q).wait_send()
    for copy in quad_out(ecopy1) + quad_out(bcopy1):
        copy.wait_send()
    for n in (1, 2, 3):
        for small in (ecopy2, ecopy3, bcopy2, bcopy3):
            small(n).wait_send()


def finish(hourly, table, out, depth):
    out[...] = hourly[...]
    depth[...] = (table[...] / table[:, HOURS : HOURS + 1])[:, :HOURS]


def body(reflectivity, scan_hour, basin_ids):
    def vmem(*shape):
        return pltpu.VMEM(shape, jnp.float32)

    def dma(*shape):
        return pltpu.SemaphoreType.DMA(shape)

    chunks = range(CHUNKS)
    scratch = [
        vmem(CHUNKS, 2, 2, 4, 4, 2, 8, 128),
        vmem(CHUNKS, 2, 2, 2, 4, 4, 8, 128),
        *[vmem(4, SLOTS[ch % 2], 4, 8, 128) for ch in chunks],
        *[vmem(4, HOURS + LOW, 4, 8, 128) for ch in chunks],
        *[vmem(4, HOURS, 8, 128) for ch in chunks],
        *[vmem(3, HOURS, 8, 128) for ch in chunks],
        vmem(2, 2, 2, 8, 128), vmem(2, 2, 2, 8, 128), vmem(HOURS, 8, 128), vmem(3, HOURS, 8, 128),
        vmem(HOURS // 4, 8, 128), vmem(3, HOURS // 4, 8, 128),
        vmem(8, 16, 128), vmem(8, 16, 128), vmem(16, 128), vmem(3, 16, 128), vmem(8, 128), vmem(3, 8, 128),
        dma(CHUNKS), dma(CHUNKS, 8), dma(CHUNKS, 8), dma(CHUNKS, 4), dma(CHUNKS, 4), dma(CHUNKS, 4), dma(CHUNKS, 4),
        dma(8), dma(8), dma(4), dma(4), dma(4), dma(4), dma(8), dma(8), dma(4), dma(4), dma(4), dma(4),
    ]
    block = pl.BlockSpec(memory_space=pltpu.VMEM)
    hourly, table = pl.pallas_call(
        kernel,
        out_shape=(
            jax.ShapeDtypeStruct((HOURS, 32, 256), jnp.float32),
            jax.ShapeDtypeStruct((8, 128), jnp.float32),
        ),
        in_specs=[pl.BlockSpec(memory_space=pl.ANY), pl.BlockSpec(memory_space=pltpu.SMEM), block],
        out_specs=(block, block),
        scratch_shapes=scratch,
        compiler_params=pltpu.CompilerParams(
            collective_id=0, has_side_effects=True, vmem_limit_bytes=52 * 1024 * 1024
        ),
    )(reflectivity.reshape(4, 2, 2, BANDS, 8, 2048), scan_hour, basin_ids.T)
    return pl.pallas_call(
        finish,
        out_shape=(
            jax.ShapeDtypeStruct((HOURS, 32, 256), jnp.float32),
            jax.ShapeDtypeStruct((8, HOURS), jnp.float32),
        ),
        in_specs=[block, block],
        out_specs=(block, block),
        compiler_params=pltpu.CompilerParams(vmem_limit_bytes=8 * 1024 * 1024),
    )(hourly, table)


def solution(mesh):
    placed = (P(("row", "col"), None, None), P(), P("row", "col"))
    return jax.shard_map(
        body,
        mesh=mesh,
        in_specs=placed,
        out_specs=(P(None, "row", "col"), P(("row", "col"), None)),
        check_vma=False,
    )
```

```python
import math

import jax
import jax.numpy as jnp
from jax import lax
from jax.experimental import pallas as pl
from jax.experimental.pallas import tpu as pltpu
from jax.sharding import PartitionSpec as P

MESH = pl.DeviceIdType.MESH
SEG = 128
HOURS = 12
BANDS = 4
CHUNKS = 8
EARLY_Z = (6, 7)
LATE_Z = (3,)
SLOTS = (4, 5)
LOW = 11
LOG2E = 1.0 / math.log(2.0)
SCALE = math.log(10.0) / 16.0 * LOG2E
SHIFT = (math.log(200.0) / 1.6 + math.log(12.0)) * LOG2E


def rain_depth(reflect):
    return jnp.exp2(reflect * SCALE - SHIFT)


def flip(value, mask):
    if mask == 0:
        return value
    if mask == 1:
        return value + 1 - 2 * (value % 2)
    if mask == 2:
        return (value + 2) % 4
    return 3 - value


def masks(parity):
    return (1, 3) if parity == 0 else (3, 1)


def device(x, y, z, c):
    return (z * 4 + (y // 2) * 2 + c, (y % 2) * 4 + x)


def kernel(refl, hours, ids, out, table_out, *scratch):
    src, got1 = scratch[:2]
    slots_of, gotz, sumz, gotq = (scratch[2 + CHUNKS * i : 2 + CHUNKS * (i + 1)] for i in range(4))
    (
        own_seg, got_seg, seg_hours, got_hours, seg_pack, got_pack, part, part_got, part_sum, part_last, row_sum, row_got,
        load_sem, send1, recv1, sendz, recvz, sendq, recvq, esend1, erecv1, esend2, erecv2, esend3, erecv3,
        bsend1, brecv1, bsend2, brecv2, bsend3, brecv3,
    ) = scratch[2 + CHUNKS * 4 : len(scratch) - 3 - len(EARLY_Z)]
    raw_z = dict(zip(EARLY_Z, scratch[len(scratch) - 3 - len(EARLY_Z) :]))
    sendr, recvr, localr = scratch[-3:]
    row, col = lax.axis_index("row"), lax.axis_index("col")
    z, c = row // 4, row % 2
    y, x = ((row // 2) % 2) * 2 + col // 4, col % 4

    barrier = pltpu.get_barrier_semaphore()
    quads = [(0, 1), (1, 0), (1, 1)]
    peers = [device(x, y, z, 1 - c)]
    for mask in (1, 3):
        for ry, rx in quads:
            for core in range(2):
                peers.append(device(flip(x, mask * rx), flip(y, mask * ry), z, core))
    for dz in (1, 2, 3):
        peers.append(device(x, y, (z + dz) % 4, c))
    for peer in peers:
        pl.semaphore_signal(barrier, inc=1, device_id=peer, device_id_type=MESH)

    def load(ch):
        m1, m2 = masks(ch % 2)
        for ry1 in range(2):
            for rx1 in range(2):
                for q in range(4):
                    dy = flip(y, (m1 * ry1) ^ (m2 * (q // 2)))
                    dx = flip(x, (m1 * rx1) ^ (m2 * (q % 2)))
                    lanes = pl.ds(pl.multiple_of(((dy % 2) * 4 + dx) * 256 + (ch % 2) * 128, 128), 128)
                    pltpu.make_async_copy(
                        refl.at[:, dy // 2, :, ch // 2, :, lanes],
                        src.at[ch, ry1, rx1, :, q],
                        load_sem.at[ch],
                    ).start()

    for ch in (0, 1) + EARLY_Z:
        load(ch)
    pl.semaphore_wait(barrier, len(peers))

    def clear():
        for ch in range(CHUNKS):
            empty = jnp.zeros(gotz[ch].shape[2:], jnp.float32)
            buf, slots = gotz[ch], SLOTS[ch % 2]

            @pl.loop(0, 4)
            def _(s):
                for k in range(HOURS + LOW):
                    if not LOW <= k < LOW + slots:
                        buf[s, k] = empty


    def copy1(ch, ry1, rx1, tc, sc):
        m1, _ = masks(ch % 2)
        block = raw_z[ch].at[:, ry1, rx1, :, tc] if ch in EARLY_Z else src.at[ch, ry1, rx1, :, :, tc]
        return pltpu.make_async_remote_copy(
            src_ref=block,
            dst_ref=got1.at[ch, ry1, rx1, sc],
            send_sem=send1.at[ch, (ry1 * 2 + rx1) * 2 + tc],
            recv_sem=recv1.at[ch, (ry1 * 2 + rx1) * 2 + sc],
            device_id=device(flip(x, m1 * rx1), flip(y, m1 * ry1), z, tc),
            device_id_type=MESH,
        )

    def step1_copies(ch, mine, which=slice(0, 7)):
        partners = [(ry1, rx1, core) for ry1, rx1 in quads for core in range(2)]
        found = []
        for ry1, rx1, core in (partners + [(0, 0, 1 - c)])[which]:
            found.append(copy1(ch, ry1, rx1, core, c) if mine else copy1(ch, ry1, rx1, c, core))
        return found

    def base_scan(ch, zz):
        return zz * 32 + (y // 2) * 16 if ch % 2 == 0 else zz * 32

    def reduce1(ch):
        m1, _ = masks(ch % 2)
        slots = SLOTS[ch % 2]

        def weights_of(zz):
            first = hours[base_scan(ch, zz)]
            weights = []
            for ry1 in range(2):
                for rx1 in range(2):
                    for core in range(2):
                        yy, xx = flip(y, m1 * ry1), flip(x, m1 * rx1)
                        cc = core if ry1 + rx1 else (c if core == 0 else 1 - c)
                        hour = hours[zz * 32 + (yy // 2) * 16 + cc * 8 + (yy % 2) * 4 + xx]
                        weights.append([jnp.where(hour - first == k, 1.0, 0.0).astype(jnp.float32) for k in range(slots)])
            return weights

        if ch not in EARLY_Z:
            fixed = weights_of(z)

        @pl.loop(0, 4)
        def _(zt):
            weights = weights_of((z - zt + 4) % 4) if ch in EARLY_Z else fixed
            for part_q in (0, 2):
                pair = pl.ds(part_q, 2)
                total = [None] * slots
                n = 0
                for ry1 in range(2):
                    for rx1 in range(2):
                        for core in range(2):
                            if ry1 + rx1:
                                raw = got1[ch, ry1, rx1, core, zt, pair]
                            elif core == 1:
                                raw = got1[ch, 0, 0, 1 - c, zt, pair]
                            elif ch in EARLY_Z:
                                raw = raw_z[ch][zt, 0, 0, pair, c]
                            else:
                                raw = src[ch, 0, 0, zt, pair, c]
                            value = rain_depth(raw)
                            for k in range(slots):
                                term = value * weights[n][k]
                                total[k] = term if total[k] is None else total[k] + term
                            n += 1
                for k in range(slots):
                    if ch in EARLY_Z:
                        gotz[ch][zt, LOW + k, pair] = total[k]
                    elif ch in LATE_Z:
                        slots_of[ch][pair, k, zt] = total[k]
                    else:
                        slots_of[ch][zt, k, pair] = total[k]

    def copyr(ch, dz):
        target_z = (z + dz) % 4
        return pltpu.make_async_remote_copy(
            src_ref=src.at[ch, :, :, target_z],
            dst_ref=raw_z[ch].at[dz],
            send_sem=sendr.at[ch, dz],
            recv_sem=recvr.at[ch, dz],
            device_id=device(x, y, target_z, c),
            device_id_type=MESH,
        )

    def copyr_own(ch):
        return pltpu.make_async_copy(src.at[ch, :, :, z], raw_z[ch].at[0], localr.at[ch])

    def startz(ch, steps=(2, 1, 3)):
        for dz in steps:
            copyr(ch, dz).start()
        if 1 in steps:
            copyr_own(ch).start()

    def copyz(ch, dz):
        target_z = (z + dz) % 4
        block = sumz[ch] if ch in LATE_Z else slots_of[ch]
        return pltpu.make_async_remote_copy(
            src_ref=block.at[target_z],
            dst_ref=gotz[ch].at[dz, pl.ds(LOW, SLOTS[ch % 2])],
            send_sem=sendz.at[ch, dz],
            recv_sem=recvz.at[ch, dz],
            device_id=device(x, y, target_z, c),
            device_id_type=MESH,
        )

    def combinez(ch):
        starts = [LOW - hours[base_scan(ch, (z - dz + 4) % 4)] for dz in range(4)]
        for h in range(HOURS):
            terms = [gotz[ch][dz, starts[dz] + h] for dz in range(4)]
            sumz[ch][:, h] = (terms[0] + terms[1]) + (terms[2] + terms[3])

    def copyq(ch, q):
        _, m2 = masks(ch % 2)
        block = slots_of[ch] if ch in LATE_Z else sumz[ch]
        return pltpu.make_async_remote_copy(
            src_ref=block.at[q],
            dst_ref=gotq[ch].at[q - 1],
            send_sem=sendq.at[ch, q],
            recv_sem=recvq.at[ch, q],
            device_id=device(flip(x, m2 * (q % 2)), flip(y, m2 * (q // 2)), z, c),
            device_id_type=MESH,
        )

    def loaded(*which):
        for ch in which:
            pltpu.make_async_copy(src.at[ch], src.at[ch], load_sem.at[ch]).wait()

    def start1(pair, which=slice(0, 7)):
        for ch in (2 * pair, 2 * pair + 1):
            if ch in EARLY_Z:
                copyr_own(ch).wait()
                for dz in (1, 2, 3):
                    copyr(ch, dz).wait_recv()
        for one, two in zip(step1_copies(2 * pair, True, which), step1_copies(2 * pair + 1, True, which)):
            one.start()
            two.start()

    def send_z(ch, block):
        for dz in (2, 1, 3):
            copyz(ch, dz).start()
        for k in range(SLOTS[ch % 2]):
            gotz[ch][0, LOW + k] = block[z, k]

    def send_q(ch):
        for q in (3, 1, 2):
            copyq(ch, q).start()

    def first(*which):
        for ch in which:
            for copy in step1_copies(ch, False):
                copy.wait_recv()
            reduce1(ch)
            if ch in EARLY_Z:
                combinez(ch)
            if ch in EARLY_Z + LATE_Z:
                send_q(ch)
            else:
                send_z(ch, slots_of[ch])

    def second(*which):
        for ch in which:
            if ch in LATE_Z:
                for q in (1, 2, 3):
                    copyq(ch, q).wait_recv()
                for zt in range(4):
                    for k in range(SLOTS[ch % 2]):
                        sumz[ch][zt, k] = (slots_of[ch][0, k, zt] + gotq[ch][0, k, zt]) + (
                            gotq[ch][1, k, zt] + gotq[ch][2, k, zt]
                        )
                send_z(ch, sumz[ch])
            else:
                for dz in (1, 2, 3):
                    copyz(ch, dz).wait_recv()
                combinez(ch)
                send_q(ch)

    def third(*which):
        for ch in which:
            band = slice(ch // 2 * 8, ch // 2 * 8 + 8)
            half = slice(ch % 2 * 128, ch % 2 * 128 + 128)
            if ch in LATE_Z:
                for dz in (1, 2, 3):
                    copyz(ch, dz).wait_recv()
                starts = [LOW - hours[base_scan(ch, (z - dz + 4) % 4)] for dz in range(4)]
            else:
                for q in (1, 2, 3):
                    copyq(ch, q).wait_recv()
            for h in range(HOURS):
                if ch in LATE_Z:
                    terms = [gotz[ch][dz, starts[dz] + h] for dz in range(4)]
                else:
                    terms = [sumz[ch][0, h]] + [gotq[ch][n, h] for n in range(3)]
                out[h, band, half] = (terms[0] + terms[1]) + (terms[2] + terms[3])

    lane = lax.broadcasted_iota(jnp.int32, (8, 128), 1)

    def own_segments():
        def one_z(zt, totals):
            totals = list(totals)
            here = lane - zt * 32
            for q in range(4):
                for ch in range(CHUNKS):
                    spot = here == q * 8 + ch
                    for n in range(8):
                        ey1, ex1, core = n // 4, (n // 2) % 2, n % 2
                        if ch % 2 == 0:
                            raw = src[ch, ey1, ex1, zt, q, core]
                        else:
                            raw = src[ch, q // 2, q % 2, zt, ey1 * 2 + ex1, core]
                        total = jnp.sum(rain_depth(raw), axis=1, keepdims=True)
                        totals[n] = jnp.where(spot, total, totals[n])
            return tuple(totals)

        totals = lax.fori_loop(0, 4, one_z, tuple(jnp.zeros((8, 128), jnp.float32) for _ in range(8)))
        for n in range(8):
            own_seg[n // 4, (n // 2) % 2, n % 2] = totals[n]

    def ecopy1(ry1, rx1, tc, sc):
        n = (ry1 * 2 + rx1) * 2
        return pltpu.make_async_remote_copy(
            src_ref=own_seg.at[ry1, rx1, tc],
            dst_ref=got_seg.at[ry1, rx1, sc],
            send_sem=esend1.at[n + tc],
            recv_sem=erecv1.at[n + sc],
            device_id=device(flip(x, rx1), flip(y, ry1), z, tc),
            device_id_type=MESH,
        )

    def ecopy2(dz):
        return pltpu.make_async_remote_copy(
            src_ref=seg_hours.at[dz],
            dst_ref=got_hours.at[dz - 1],
            send_sem=esend2.at[dz],
            recv_sem=erecv2.at[dz],
            device_id=device(x, y, (z + dz) % 4, c),
            device_id_type=MESH,
        )

    def ecopy3(q):
        return pltpu.make_async_remote_copy(
            src_ref=seg_pack,
            dst_ref=got_pack.at[q - 1],
            send_sem=esend3.at[q],
            recv_sem=erecv3.at[q],
            device_id=device(flip(x, 3 * (q % 2)), flip(y, 3 * (q // 2)), z, c),
            device_id_type=MESH,
        )

    def quad_out(copy):
        found = [copy(ry1, rx1, core, c) for ry1, rx1 in quads for core in range(2)]
        return found + [copy(0, 0, 1 - c, c)]

    def quad_in(copy):
        found = [copy(ry1, rx1, c, core) for ry1, rx1 in quads for core in range(2)]
        return found + [copy(0, 0, c, 1 - c)]

    def segments1():
        loaded(*[ch for ch in range(2, CHUNKS) if ch not in EARLY_Z])
        own_segments()
        for copy in quad_out(ecopy1):
            copy.start()

    def segments2():
        for copy in quad_in(ecopy1):
            copy.wait_recv()
        totals = [None] * HOURS
        for ry1 in range(2):
            for rx1 in range(2):
                for core in range(2):
                    yy, xx = flip(y, ry1), flip(x, rx1)
                    if ry1 + rx1:
                        cc, value = core, got_seg[ry1, rx1, core]
                    elif core == 0:
                        cc, value = c, own_seg[0, 0, c]
                    else:
                        cc, value = 1 - c, got_seg[0, 0, 1 - c]
                    hour = hours[z * 32 + (yy // 2) * 16 + cc * 8 + (yy % 2) * 4 + xx]
                    for h in range(HOURS):
                        term = value * jnp.where(hour == h, 1.0, 0.0).astype(jnp.float32)
                        totals[h] = term if totals[h] is None else totals[h] + term
        for dz in (2, 1, 3, 0):
            for k in range(HOURS // 4):
                packed = jnp.zeros((8, 128), jnp.float32)
                for h in range(4 * k, 4 * k + 4):
                    value = jnp.where(lane // 32 == (z + dz) % 4, totals[h], 0.0)
                    value = value + pltpu.roll(value, 64, 1)
                    value = value + pltpu.roll(value, 32, 1)
                    packed = jnp.where(lane // 32 == h % 4, value, packed)
                seg_hours[dz, k] = packed
        for dz in (2, 1, 3):
            ecopy2(dz).start()

    def segments3():
        for dz in (1, 2, 3):
            ecopy2(dz).wait_recv()
        for k in range(HOURS // 4):
            seg_pack[k] = (seg_hours[0, k] + got_hours[0, k]) + (got_hours[1, k] + got_hours[2, k])
        for q in (3, 1, 2):
            ecopy3(q).start()

    def shares():
        for q in (1, 2, 3):
            ecopy3(q).wait_recv()
        table = []
        for k in range(HOURS // 4):
            value = seg_pack[k]
            for q in (1, 2, 3):
                value = value + pltpu.roll(got_pack[q - 1, k], 128 - 8 * q, 1)
            table.append(value)
        tile_rows = out.shape[1]
        wide = lax.broadcasted_iota(jnp.int32, (tile_rows, 128), 1)
        rank = lax.broadcasted_iota(jnp.int32, (128, tile_rows), 0)
        oz, orx2, ory2 = rank % 4, (rank // 4) % 2, (rank // 8) % 2
        oc, orx1, ory1 = (rank // 16) % 2, (rank // 32) % 2, rank // 64

        def flip_each(value, bit, mask):
            return jnp.where(bit == 1, flip(value, mask), value)

        ox = flip_each(flip_each(jnp.full_like(rank, x), orx1, 1), orx2, 3)
        oy = flip_each(flip_each(jnp.full_like(rank, y), ory1, 1), ory2, 3)
        owner = (oz * 4 + (oy // 2) * 2 + oc) * 8 + (oy % 2) * 4 + ox
        square = (tile_rows, tile_rows)
        diagonal = lax.broadcasted_iota(jnp.int32, square, 0) == lax.broadcasted_iota(jnp.int32, square, 1)
        share = jnp.zeros((128, 128), jnp.float32)
        for g in range(2):
            bands = []
            for j in range(BANDS):
                value = jnp.where(lane % 16 == HOURS, float(SEG), 0.0)
                for h in range(HOURS):
                    at = (h % 4) * 32 + j * 2 + g
                    value = jnp.where(lane % 16 == h, table[h // 4][:, at : at + 1], value)
                bands.append(value)
            value = jnp.concatenate(bands, axis=0)
            names = ids[g : g + 1, :]
            place = (names % 8).astype(jnp.float32)
            place = jnp.sum(jnp.where(diagonal, place, 0.0), axis=1, keepdims=True)
            value = jnp.where((wide // 16).astype(jnp.float32) == place, value, 0.0)
            chosen = jnp.where(owner == names // 8, 1.0, 0.0)
            share = share + jnp.dot(
                chosen, value, precision=lax.Precision.HIGHEST, preferred_element_type=jnp.float32
            )
        part[...] = share.reshape(8, 16, 128)
        for copy in quad_out(bcopy1):
            copy.start()

    def bcopy1(ry1, rx1, tc, sc):
        n = (ry1 * 2 + rx1) * 2
        return pltpu.make_async_remote_copy(
            src_ref=part.at[n + tc],
            dst_ref=part_got.at[n + sc],
            send_sem=bsend1.at[n + tc],
            recv_sem=brecv1.at[n + sc],
            device_id=device(flip(x, rx1), flip(y, ry1), z, tc),
            device_id_type=MESH,
        )

    def bcopy2(q):
        return pltpu.make_async_remote_copy(
            src_ref=part_sum,
            dst_ref=part_last.at[q - 1],
            send_sem=bsend2.at[q],
            recv_sem=brecv2.at[q],
            device_id=device(flip(x, 3 * (q % 2)), flip(y, 3 * (q // 2)), z, c),
            device_id_type=MESH,
        )

    def bcopy3(dz):
        return pltpu.make_async_remote_copy(
            src_ref=row_sum,
            dst_ref=row_got.at[dz - 1],
            send_sem=bsend3.at[dz],
            recv_sem=brecv3.at[dz],
            device_id=device(x, y, (z + dz) % 4, c),
            device_id_type=MESH,
        )

    def shares2():
        for copy in quad_in(bcopy1):
            copy.wait_recv()
        summed = part[c] + part_got[1 - c]
        for ry1, rx1 in quads:
            for core in range(2):
                summed = summed + part_got[(ry1 * 2 + rx1) * 2 + core]
        part_sum[...] = summed
        for q in (3, 1, 2):
            bcopy2(q).start()

    def shares3():
        for q in (1, 2, 3):
            bcopy2(q).wait_recv()
        row_sum[...] = jnp.zeros((8, 128), jnp.float32)
        row_sum[0:4] = (part_sum[0:4] + part_last[0, 4:8]) + (part_last[1, 8:12] + part_last[2, 12:16])
        for dz in (2, 1, 3):
            bcopy3(dz).start()

    def shares4():
        final = row_sum[pl.ds(z, 1), :]
        for dz in (1, 2, 3):
            bcopy3(dz).wait_recv()
        for dz in (1, 2, 3):
            final = final + row_got[dz - 1, pl.ds(z, 1), :]
        row8 = lax.broadcasted_iota(jnp.int32, (8, 128), 0)
        spread = jnp.where(lane // 16 == row8, jnp.broadcast_to(final, (8, 128)), 0.0)
        lane_in = lax.broadcasted_iota(jnp.int32, (128, 128), 0)
        lane_out = lax.broadcasted_iota(jnp.int32, (128, 128), 1)
        pick = jnp.where(lane_in % 16 == lane_out, 1.0, 0.0)
        table_out[...] = jnp.dot(
            spread, pick, precision=lax.Precision.HIGHEST, preferred_element_type=jnp.float32
        )

    loaded(0, 1)
    start1(0, slice(0, 5))
    for ch in range(2, CHUNKS):
        if ch not in EARLY_Z:
            load(ch)
    loaded(*EARLY_Z)
    startz(6)
    startz(7, (2,))
    segments1()
    start1(0, slice(5, 7))
    start1(1)
    clear()
    segments2()
    startz(7, (1, 3))
    first(0)
    first(1)
    segments3()
    start1(2)
    shares()
    start1(3)
    first(3)
    first(2)
    second(0)
    shares2()
    first(4)
    second(1)
    first(5)
    second(2)
    second(4)
    first(7)
    first(6)
    third(0)
    shares3()
    second(3)
    second(5)
    third(2)
    shares4()
    third(1)
    third(4)
    third(3)
    third(7)
    third(6)
    third(5)

    for ch in range(CHUNKS):
        for copy in step1_copies(ch, True):
            copy.wait_send()
        for dz in (1, 2, 3):
            (copyr if ch in EARLY_Z else copyz)(ch, dz).wait_send()
        for q in (1, 2, 3):
            copyq(ch, q).wait_send()
    for copy in quad_out(ecopy1) + quad_out(bcopy1):
        copy.wait_send()
    for n in (1, 2, 3):
        for small in (ecopy2, ecopy3, bcopy2, bcopy3):
            small(n).wait_send()


def finish(hourly, table, out, depth):
    out[...] = hourly[...]
    depth[...] = (table[...] / table[:, HOURS : HOURS + 1])[:, :HOURS]


def body(reflectivity, scan_hour, basin_ids):
    def vmem(*shape):
        return pltpu.VMEM(shape, jnp.float32)

    def dma(*shape):
        return pltpu.SemaphoreType.DMA(shape)

    chunks = range(CHUNKS)
    scratch = [
        vmem(CHUNKS, 2, 2, 4, 4, 2, 8, 128),
        vmem(CHUNKS, 2, 2, 2, 4, 4, 8, 128),
        *[vmem(4, 1 if ch in EARLY_Z else SLOTS[ch % 2], 4, 8, 128) for ch in chunks],
        *[vmem(4, HOURS + LOW, *((8, 128) if ch in LATE_Z else (4, 8, 128))) for ch in chunks],
        *[vmem(4, SLOTS[1] if ch in LATE_Z else HOURS, 8, 128) for ch in chunks],
        *[vmem(3, *((SLOTS[1], 4) if ch in LATE_Z else (HOURS,)), 8, 128) for ch in chunks],
        vmem(2, 2, 2, 8, 128), vmem(2, 2, 2, 8, 128), vmem(4, HOURS // 4, 8, 128), vmem(3, HOURS // 4, 8, 128),
        vmem(HOURS // 4, 8, 128), vmem(3, HOURS // 4, 8, 128),
        vmem(8, 16, 128), vmem(8, 16, 128), vmem(16, 128), vmem(3, 16, 128), vmem(8, 128), vmem(3, 8, 128),
        dma(CHUNKS), dma(CHUNKS, 8), dma(CHUNKS, 8), dma(CHUNKS, 4), dma(CHUNKS, 4), dma(CHUNKS, 4), dma(CHUNKS, 4),
        dma(8), dma(8), dma(4), dma(4), dma(4), dma(4), dma(8), dma(8), dma(4), dma(4), dma(4), dma(4),
        *[vmem(4, 2, 2, 4, 2, 8, 128) for ch in EARLY_Z],
        dma(CHUNKS, 4), dma(CHUNKS, 4), dma(CHUNKS),
    ]
    block = pl.BlockSpec(memory_space=pltpu.VMEM)
    hourly, table = pl.pallas_call(
        kernel,
        out_shape=(
            jax.ShapeDtypeStruct((HOURS, 32, 256), jnp.float32),
            jax.ShapeDtypeStruct((8, 128), jnp.float32),
        ),
        in_specs=[pl.BlockSpec(memory_space=pl.ANY), pl.BlockSpec(memory_space=pltpu.SMEM), block],
        out_specs=(block, block),
        scratch_shapes=scratch,
        compiler_params=pltpu.CompilerParams(
            collective_id=0, has_side_effects=True, vmem_limit_bytes=52 * 1024 * 1024
        ),
    )(reflectivity.reshape(4, 2, 2, BANDS, 8, 2048), scan_hour, basin_ids.T)
    return pl.pallas_call(
        finish,
        out_shape=(
            jax.ShapeDtypeStruct((HOURS, 32, 256), jnp.float32),
            jax.ShapeDtypeStruct((8, HOURS), jnp.float32),
        ),
        in_specs=[block, block],
        out_specs=(block, block),
        compiler_params=pltpu.CompilerParams(vmem_limit_bytes=8 * 1024 * 1024),
    )(hourly, table)


def solution(mesh):
    placed = (P(("row", "col"), None, None), P(), P("row", "col"))
    return jax.shard_map(
        body,
        mesh=mesh,
        in_specs=placed,
        out_specs=(P(None, "row", "col"), P(("row", "col"), None)),
        check_vma=False,
    )
```

```python
import math

import jax
import jax.numpy as jnp
from jax import lax
from jax.experimental import pallas as pl
from jax.experimental.pallas import tpu as pltpu
from jax.sharding import PartitionSpec as P

MESH = pl.DeviceIdType.MESH
SEG = 128
HOURS = 12
BANDS = 4
CHUNKS = 8
EARLY_Z = (6, 7)
LATE_Z = (3,)
SLOTS = (4, 5)
LOW = 11
LOG2E = 1.0 / math.log(2.0)
SCALE = math.log(10.0) / 16.0 * LOG2E
SHIFT = (math.log(200.0) / 1.6 + math.log(12.0)) * LOG2E


def rain_depth(reflect):
    return jnp.exp2(reflect * SCALE - SHIFT)


def flip(value, mask):
    if mask == 0:
        return value
    if mask == 1:
        return value + 1 - 2 * (value % 2)
    if mask == 2:
        return (value + 2) % 4
    return 3 - value


def masks(parity):
    return (1, 3) if parity == 0 else (3, 1)


def device(x, y, z, c):
    return (z * 4 + (y // 2) * 2 + c, (y % 2) * 4 + x)


def kernel(refl, hours_in, ids_in, out, table_out, *scratch):
    src, got1 = scratch[:2]
    slots_of, gotz, sumz, gotq = (scratch[2 + CHUNKS * i : 2 + CHUNKS * (i + 1)] for i in range(4))
    (
        own_seg, got_seg, seg_hours, got_hours, seg_pack, got_pack, part, part_got, part_sum, part_last, row_sum, row_got,
        load_sem, send1, recv1, sendz, recvz, sendq, recvq, esend1, erecv1, esend2, erecv2, esend3, erecv3,
        bsend1, brecv1, bsend2, brecv2, bsend3, brecv3,
    ) = scratch[2 + CHUNKS * 4 : len(scratch) - 6 - len(EARLY_Z)]
    raw_z = dict(zip(EARLY_Z, scratch[len(scratch) - 6 - len(EARLY_Z) :]))
    sendr, recvr, localr, hours, ids, table_sem = scratch[-6:]
    row, col = lax.axis_index("row"), lax.axis_index("col")
    z, c = row // 4, row % 2
    y, x = ((row // 2) % 2) * 2 + col // 4, col % 4

    barrier = pltpu.get_barrier_semaphore()
    quads = [(0, 1), (1, 0), (1, 1)]
    peers = [device(x, y, z, 1 - c)]
    for mask in (1, 3):
        for ry, rx in quads:
            for core in range(2):
                peers.append(device(flip(x, mask * rx), flip(y, mask * ry), z, core))
    for dz in (1, 2, 3):
        peers.append(device(x, y, (z + dz) % 4, c))
    for peer in peers:
        pl.semaphore_signal(barrier, inc=1, device_id=peer, device_id_type=MESH)

    fetches = [
        pltpu.make_async_copy(hours_in, hours, table_sem.at[0]),
        pltpu.make_async_copy(ids_in, ids, table_sem.at[1]),
    ]

    def load(ch):
        m1, m2 = masks(ch % 2)
        for ry1 in range(2):
            for rx1 in range(2):
                for q in range(4):
                    dy = flip(y, (m1 * ry1) ^ (m2 * (q // 2)))
                    dx = flip(x, (m1 * rx1) ^ (m2 * (q % 2)))
                    lanes = pl.ds(pl.multiple_of(((dy % 2) * 4 + dx) * 256 + (ch % 2) * 128, 128), 128)
                    pltpu.make_async_copy(
                        refl.at[:, dy // 2, :, ch // 2, :, lanes],
                        src.at[ch, ry1, rx1, :, q],
                        load_sem.at[ch],
                    ).start()

    for ch in (0, 1) + EARLY_Z:
        load(ch)
    for copy in fetches:
        copy.start()
    pl.semaphore_wait(barrier, len(peers))

    def clear():
        for ch in range(CHUNKS):
            empty = jnp.zeros(gotz[ch].shape[2:], jnp.float32)
            buf, slots = gotz[ch], SLOTS[ch % 2]

            @pl.loop(0, 4)
            def _(s):
                for k in range(HOURS + LOW):
                    if not LOW <= k < LOW + slots:
                        buf[s, k] = empty


    def copy1(ch, ry1, rx1, tc, sc):
        m1, _ = masks(ch % 2)
        block = raw_z[ch].at[:, ry1, rx1, :, tc] if ch in EARLY_Z else src.at[ch, ry1, rx1, :, :, tc]
        return pltpu.make_async_remote_copy(
            src_ref=block,
            dst_ref=got1.at[ch, ry1, rx1, sc],
            send_sem=send1.at[ch, (ry1 * 2 + rx1) * 2 + tc],
            recv_sem=recv1.at[ch, (ry1 * 2 + rx1) * 2 + sc],
            device_id=device(flip(x, m1 * rx1), flip(y, m1 * ry1), z, tc),
            device_id_type=MESH,
        )

    def step1_copies(ch, mine, which=slice(0, 7)):
        partners = [(ry1, rx1, core) for ry1, rx1 in quads for core in range(2)]
        found = []
        for ry1, rx1, core in (partners + [(0, 0, 1 - c)])[which]:
            found.append(copy1(ch, ry1, rx1, core, c) if mine else copy1(ch, ry1, rx1, c, core))
        return found

    def base_scan(ch, zz):
        return zz * 32 + (y // 2) * 16 if ch % 2 == 0 else zz * 32

    def reduce1(ch):
        m1, _ = masks(ch % 2)
        slots = SLOTS[ch % 2]

        def weights_of(zz):
            first = hours[base_scan(ch, zz)]
            weights = []
            for ry1 in range(2):
                for rx1 in range(2):
                    for core in range(2):
                        yy, xx = flip(y, m1 * ry1), flip(x, m1 * rx1)
                        cc = core if ry1 + rx1 else (c if core == 0 else 1 - c)
                        hour = hours[zz * 32 + (yy // 2) * 16 + cc * 8 + (yy % 2) * 4 + xx]
                        weights.append([jnp.where(hour - first == k, 1.0, 0.0).astype(jnp.float32) for k in range(slots)])
            return weights

        if ch not in EARLY_Z:
            fixed = weights_of(z)

        @pl.loop(0, 4)
        def _(zt):
            weights = weights_of((z - zt + 4) % 4) if ch in EARLY_Z else fixed
            for part_q in (0, 2):
                pair = pl.ds(part_q, 2)
                total = [None] * slots
                n = 0
                for ry1 in range(2):
                    for rx1 in range(2):
                        for core in range(2):
                            if ry1 + rx1:
                                raw = got1[ch, ry1, rx1, core, zt, pair]
                            elif core == 1:
                                raw = got1[ch, 0, 0, 1 - c, zt, pair]
                            elif ch in EARLY_Z:
                                raw = raw_z[ch][zt, 0, 0, pair, c]
                            else:
                                raw = src[ch, 0, 0, zt, pair, c]
                            value = rain_depth(raw)
                            for k in range(slots):
                                term = value * weights[n][k]
                                total[k] = term if total[k] is None else total[k] + term
                            n += 1
                for k in range(slots):
                    if ch in EARLY_Z:
                        gotz[ch][zt, LOW + k, pair] = total[k]
                    elif ch in LATE_Z:
                        slots_of[ch][pair, k, zt] = total[k]
                    else:
                        slots_of[ch][zt, k, pair] = total[k]

    def copyr(ch, dz):
        target_z = (z + dz) % 4
        return pltpu.make_async_remote_copy(
            src_ref=src.at[ch, :, :, target_z],
            dst_ref=raw_z[ch].at[dz],
            send_sem=sendr.at[ch, dz],
            recv_sem=recvr.at[ch, dz],
            device_id=device(x, y, target_z, c),
            device_id_type=MESH,
        )

    def copyr_own(ch):
        return pltpu.make_async_copy(src.at[ch, :, :, z], raw_z[ch].at[0], localr.at[ch])

    def startz(ch, steps=(2, 1, 3)):
        for dz in steps:
            copyr(ch, dz).start()
        if 1 in steps:
            copyr_own(ch).start()

    def copyz(ch, dz):
        target_z = (z + dz) % 4
        block = sumz[ch] if ch in LATE_Z else slots_of[ch]
        return pltpu.make_async_remote_copy(
            src_ref=block.at[target_z],
            dst_ref=gotz[ch].at[dz, pl.ds(LOW, SLOTS[ch % 2])],
            send_sem=sendz.at[ch, dz],
            recv_sem=recvz.at[ch, dz],
            device_id=device(x, y, target_z, c),
            device_id_type=MESH,
        )

    def combinez(ch):
        starts = [LOW - hours[base_scan(ch, (z - dz + 4) % 4)] for dz in range(4)]
        for h in range(HOURS):
            terms = [gotz[ch][dz, starts[dz] + h] for dz in range(4)]
            sumz[ch][:, h] = (terms[0] + terms[1]) + (terms[2] + terms[3])

    def copyq(ch, q):
        _, m2 = masks(ch % 2)
        block = slots_of[ch] if ch in LATE_Z else sumz[ch]
        return pltpu.make_async_remote_copy(
            src_ref=block.at[q],
            dst_ref=gotq[ch].at[q - 1],
            send_sem=sendq.at[ch, q],
            recv_sem=recvq.at[ch, q],
            device_id=device(flip(x, m2 * (q % 2)), flip(y, m2 * (q // 2)), z, c),
            device_id_type=MESH,
        )

    def loaded(*which):
        for ch in which:
            pltpu.make_async_copy(src.at[ch], src.at[ch], load_sem.at[ch]).wait()

    def start1(pair, which=slice(0, 7)):
        for ch in (2 * pair, 2 * pair + 1):
            if ch in EARLY_Z:
                copyr_own(ch).wait()
                for dz in (1, 2, 3):
                    copyr(ch, dz).wait_recv()
        for one, two in zip(step1_copies(2 * pair, True, which), step1_copies(2 * pair + 1, True, which)):
            one.start()
            two.start()

    def send_z(ch, block):
        for dz in (2, 1, 3):
            copyz(ch, dz).start()
        for k in range(SLOTS[ch % 2]):
            gotz[ch][0, LOW + k] = block[z, k]

    def send_q(ch):
        for q in (3, 1, 2):
            copyq(ch, q).start()

    def first(*which):
        for ch in which:
            for copy in step1_copies(ch, False):
                copy.wait_recv()
            reduce1(ch)
            if ch in EARLY_Z:
                combinez(ch)
            if ch in EARLY_Z + LATE_Z:
                send_q(ch)
            else:
                send_z(ch, slots_of[ch])

    def second(*which):
        for ch in which:
            if ch in LATE_Z:
                for q in (1, 2, 3):
                    copyq(ch, q).wait_recv()
                for zt in range(4):
                    for k in range(SLOTS[ch % 2]):
                        sumz[ch][zt, k] = (slots_of[ch][0, k, zt] + gotq[ch][0, k, zt]) + (
                            gotq[ch][1, k, zt] + gotq[ch][2, k, zt]
                        )
                send_z(ch, sumz[ch])
            else:
                for dz in (1, 2, 3):
                    copyz(ch, dz).wait_recv()
                combinez(ch)
                send_q(ch)

    def third(*which):
        for ch in which:
            band = slice(ch // 2 * 8, ch // 2 * 8 + 8)
            half = slice(ch % 2 * 128, ch % 2 * 128 + 128)
            if ch in LATE_Z:
                for dz in (1, 2, 3):
                    copyz(ch, dz).wait_recv()
                starts = [LOW - hours[base_scan(ch, (z - dz + 4) % 4)] for dz in range(4)]
            else:
                for q in (1, 2, 3):
                    copyq(ch, q).wait_recv()
            for h in range(HOURS):
                if ch in LATE_Z:
                    terms = [gotz[ch][dz, starts[dz] + h] for dz in range(4)]
                else:
                    terms = [sumz[ch][0, h]] + [gotq[ch][n, h] for n in range(3)]
                out[h, band, half] = (terms[0] + terms[1]) + (terms[2] + terms[3])

    lane = lax.broadcasted_iota(jnp.int32, (8, 128), 1)

    def own_segments():
        def one_z(zt, totals):
            totals = list(totals)
            here = lane - zt * 32
            for q in range(4):
                for ch in range(CHUNKS):
                    spot = here == q * 8 + ch
                    for n in range(8):
                        ey1, ex1, core = n // 4, (n // 2) % 2, n % 2
                        if ch % 2 == 0:
                            raw = src[ch, ey1, ex1, zt, q, core]
                        else:
                            raw = src[ch, q // 2, q % 2, zt, ey1 * 2 + ex1, core]
                        total = jnp.sum(rain_depth(raw), axis=1, keepdims=True)
                        totals[n] = jnp.where(spot, total, totals[n])
            return tuple(totals)

        totals = lax.fori_loop(0, 4, one_z, tuple(jnp.zeros((8, 128), jnp.float32) for _ in range(8)))
        for n in range(8):
            own_seg[n // 4, (n // 2) % 2, n % 2] = totals[n]

    def ecopy1(ry1, rx1, tc, sc):
        n = (ry1 * 2 + rx1) * 2
        return pltpu.make_async_remote_copy(
            src_ref=own_seg.at[ry1, rx1, tc],
            dst_ref=got_seg.at[ry1, rx1, sc],
            send_sem=esend1.at[n + tc],
            recv_sem=erecv1.at[n + sc],
            device_id=device(flip(x, rx1), flip(y, ry1), z, tc),
            device_id_type=MESH,
        )

    def ecopy2(dz):
        return pltpu.make_async_remote_copy(
            src_ref=seg_hours.at[dz],
            dst_ref=got_hours.at[dz - 1],
            send_sem=esend2.at[dz],
            recv_sem=erecv2.at[dz],
            device_id=device(x, y, (z + dz) % 4, c),
            device_id_type=MESH,
        )

    def ecopy3(q):
        return pltpu.make_async_remote_copy(
            src_ref=seg_pack,
            dst_ref=got_pack.at[q - 1],
            send_sem=esend3.at[q],
            recv_sem=erecv3.at[q],
            device_id=device(flip(x, 3 * (q % 2)), flip(y, 3 * (q // 2)), z, c),
            device_id_type=MESH,
        )

    def quad_out(copy):
        found = [copy(ry1, rx1, core, c) for ry1, rx1 in quads for core in range(2)]
        return found + [copy(0, 0, 1 - c, c)]

    def quad_in(copy):
        found = [copy(ry1, rx1, c, core) for ry1, rx1 in quads for core in range(2)]
        return found + [copy(0, 0, c, 1 - c)]

    def segments1():
        loaded(*[ch for ch in range(2, CHUNKS) if ch not in EARLY_Z])
        own_segments()
        for copy in quad_out(ecopy1):
            copy.start()

    def segments2():
        for copy in quad_in(ecopy1):
            copy.wait_recv()
        totals = [None] * HOURS
        for ry1 in range(2):
            for rx1 in range(2):
                for core in range(2):
                    yy, xx = flip(y, ry1), flip(x, rx1)
                    if ry1 + rx1:
                        cc, value = core, got_seg[ry1, rx1, core]
                    elif core == 0:
                        cc, value = c, own_seg[0, 0, c]
                    else:
                        cc, value = 1 - c, got_seg[0, 0, 1 - c]
                    hour = hours[z * 32 + (yy // 2) * 16 + cc * 8 + (yy % 2) * 4 + xx]
                    for h in range(HOURS):
                        term = value * jnp.where(hour == h, 1.0, 0.0).astype(jnp.float32)
                        totals[h] = term if totals[h] is None else totals[h] + term
        for dz in (2, 1, 3, 0):
            for k in range(HOURS // 4):
                packed = jnp.zeros((8, 128), jnp.float32)
                for h in range(4 * k, 4 * k + 4):
                    value = jnp.where(lane // 32 == (z + dz) % 4, totals[h], 0.0)
                    value = value + pltpu.roll(value, 64, 1)
                    value = value + pltpu.roll(value, 32, 1)
                    packed = jnp.where(lane // 32 == h % 4, value, packed)
                seg_hours[dz, k] = packed
        for dz in (2, 1, 3):
            ecopy2(dz).start()

    def segments3():
        for dz in (1, 2, 3):
            ecopy2(dz).wait_recv()
        for k in range(HOURS // 4):
            seg_pack[k] = (seg_hours[0, k] + got_hours[0, k]) + (got_hours[1, k] + got_hours[2, k])
        for q in (3, 1, 2):
            ecopy3(q).start()

    def shares():
        for q in (1, 2, 3):
            ecopy3(q).wait_recv()
        table = []
        for k in range(HOURS // 4):
            value = seg_pack[k]
            for q in (1, 2, 3):
                value = value + pltpu.roll(got_pack[q - 1, k], 128 - 8 * q, 1)
            table.append(value)
        tile_rows = out.shape[1]
        wide = lax.broadcasted_iota(jnp.int32, (tile_rows, 128), 1)
        rank = lax.broadcasted_iota(jnp.int32, (128, tile_rows), 0)
        oz, orx2, ory2 = rank % 4, (rank // 4) % 2, (rank // 8) % 2
        oc, orx1, ory1 = (rank // 16) % 2, (rank // 32) % 2, rank // 64

        def flip_each(value, bit, mask):
            return jnp.where(bit == 1, flip(value, mask), value)

        ox = flip_each(flip_each(jnp.full_like(rank, x), orx1, 1), orx2, 3)
        oy = flip_each(flip_each(jnp.full_like(rank, y), ory1, 1), ory2, 3)
        owner = (oz * 4 + (oy // 2) * 2 + oc) * 8 + (oy % 2) * 4 + ox
        square = (tile_rows, tile_rows)
        diagonal = lax.broadcasted_iota(jnp.int32, square, 0) == lax.broadcasted_iota(jnp.int32, square, 1)
        share = jnp.zeros((128, 128), jnp.float32)
        for g in range(2):
            bands = []
            for j in range(BANDS):
                value = jnp.where(lane % 16 == HOURS, float(SEG), 0.0)
                for h in range(HOURS):
                    at = (h % 4) * 32 + j * 2 + g
                    value = jnp.where(lane % 16 == h, table[h // 4][:, at : at + 1], value)
                bands.append(value)
            value = jnp.concatenate(bands, axis=0)
            names = ids[g : g + 1, :]
            place = (names % 8).astype(jnp.float32)
            place = jnp.sum(jnp.where(diagonal, place, 0.0), axis=1, keepdims=True)
            value = jnp.where((wide // 16).astype(jnp.float32) == place, value, 0.0)
            chosen = jnp.where(owner == names // 8, 1.0, 0.0)
            share = share + jnp.dot(
                chosen, value, precision=lax.Precision.HIGHEST, preferred_element_type=jnp.float32
            )
        part[...] = share.reshape(8, 16, 128)
        for copy in quad_out(bcopy1):
            copy.start()

    def bcopy1(ry1, rx1, tc, sc):
        n = (ry1 * 2 + rx1) * 2
        return pltpu.make_async_remote_copy(
            src_ref=part.at[n + tc],
            dst_ref=part_got.at[n + sc],
            send_sem=bsend1.at[n + tc],
            recv_sem=brecv1.at[n + sc],
            device_id=device(flip(x, rx1), flip(y, ry1), z, tc),
            device_id_type=MESH,
        )

    def bcopy2(q):
        return pltpu.make_async_remote_copy(
            src_ref=part_sum,
            dst_ref=part_last.at[q - 1],
            send_sem=bsend2.at[q],
            recv_sem=brecv2.at[q],
            device_id=device(flip(x, 3 * (q % 2)), flip(y, 3 * (q // 2)), z, c),
            device_id_type=MESH,
        )

    def bcopy3(dz):
        return pltpu.make_async_remote_copy(
            src_ref=row_sum,
            dst_ref=row_got.at[dz - 1],
            send_sem=bsend3.at[dz],
            recv_sem=brecv3.at[dz],
            device_id=device(x, y, (z + dz) % 4, c),
            device_id_type=MESH,
        )

    def shares2():
        for copy in quad_in(bcopy1):
            copy.wait_recv()
        summed = part[c] + part_got[1 - c]
        for ry1, rx1 in quads:
            for core in range(2):
                summed = summed + part_got[(ry1 * 2 + rx1) * 2 + core]
        part_sum[...] = summed
        for q in (3, 1, 2):
            bcopy2(q).start()

    def shares3():
        for q in (1, 2, 3):
            bcopy2(q).wait_recv()
        row_sum[...] = jnp.zeros((8, 128), jnp.float32)
        row_sum[0:4] = (part_sum[0:4] + part_last[0, 4:8]) + (part_last[1, 8:12] + part_last[2, 12:16])
        for dz in (2, 1, 3):
            bcopy3(dz).start()

    def shares4():
        final = row_sum[pl.ds(z, 1), :]
        for dz in (1, 2, 3):
            bcopy3(dz).wait_recv()
        for dz in (1, 2, 3):
            final = final + row_got[dz - 1, pl.ds(z, 1), :]
        row8 = lax.broadcasted_iota(jnp.int32, (8, 128), 0)
        spread = jnp.where(lane // 16 == row8, jnp.broadcast_to(final, (8, 128)), 0.0)
        lane_in = lax.broadcasted_iota(jnp.int32, (128, 128), 0)
        lane_out = lax.broadcasted_iota(jnp.int32, (128, 128), 1)
        pick = jnp.where(lane_in % 16 == lane_out, 1.0, 0.0)
        table_out[...] = jnp.dot(
            spread, pick, precision=lax.Precision.HIGHEST, preferred_element_type=jnp.float32
        )

    def sent():
        for ch in range(CHUNKS):
            for copy in step1_copies(ch, True):
                copy.wait_send()
            for dz in (1, 2, 3):
                (copyr if ch in EARLY_Z else copyz)(ch, dz).wait_send()
        for copy in quad_out(ecopy1) + quad_out(bcopy1):
            copy.wait_send()
        for n in (1, 2, 3):
            for small in (ecopy2, ecopy3, bcopy2, bcopy3):
                small(n).wait_send()

    loaded(0, 1)
    start1(0, slice(0, 5))
    for ch in range(2, CHUNKS):
        if ch not in EARLY_Z:
            load(ch)
    loaded(*EARLY_Z)
    startz(6)
    startz(7, (2,))
    segments1()
    for copy in fetches:
        copy.wait()
    start1(0, slice(5, 7))
    start1(1)
    clear()
    segments2()
    startz(7, (1, 3))
    first(0)
    first(1)
    segments3()
    start1(2)
    shares()
    start1(3)
    first(3)
    first(2)
    second(0)
    shares2()
    first(4)
    second(1)
    first(5)
    second(2)
    second(4)
    first(7)
    first(6)
    third(0)
    shares3()
    second(3)
    second(5)
    third(2)
    shares4()
    third(1)
    third(4)
    sent()
    third(3)
    third(7)
    third(6)
    third(5)

    for ch in range(CHUNKS):
        for q in (1, 2, 3):
            copyq(ch, q).wait_send()


def finish(hourly, table, out, depth):
    out[...] = hourly[...]
    depth[...] = (table[...] / table[:, HOURS : HOURS + 1])[:, :HOURS]


def body(reflectivity, scan_hour, basin_ids):
    def vmem(*shape):
        return pltpu.VMEM(shape, jnp.float32)

    def dma(*shape):
        return pltpu.SemaphoreType.DMA(shape)

    chunks = range(CHUNKS)
    scratch = [
        vmem(CHUNKS, 2, 2, 4, 4, 2, 8, 128),
        vmem(CHUNKS, 2, 2, 2, 4, 4, 8, 128),
        *[vmem(4, 1 if ch in EARLY_Z else SLOTS[ch % 2], 4, 8, 128) for ch in chunks],
        *[vmem(4, HOURS + LOW, *((8, 128) if ch in LATE_Z else (4, 8, 128))) for ch in chunks],
        *[vmem(4, SLOTS[1] if ch in LATE_Z else HOURS, 8, 128) for ch in chunks],
        *[vmem(3, *((SLOTS[1], 4) if ch in LATE_Z else (HOURS,)), 8, 128) for ch in chunks],
        vmem(2, 2, 2, 8, 128), vmem(2, 2, 2, 8, 128), vmem(4, HOURS // 4, 8, 128), vmem(3, HOURS // 4, 8, 128),
        vmem(HOURS // 4, 8, 128), vmem(3, HOURS // 4, 8, 128),
        vmem(8, 16, 128), vmem(8, 16, 128), vmem(16, 128), vmem(3, 16, 128), vmem(8, 128), vmem(3, 8, 128),
        dma(CHUNKS), dma(CHUNKS, 8), dma(CHUNKS, 8), dma(CHUNKS, 4), dma(CHUNKS, 4), dma(CHUNKS, 4), dma(CHUNKS, 4),
        dma(8), dma(8), dma(4), dma(4), dma(4), dma(4), dma(8), dma(8), dma(4), dma(4), dma(4), dma(4),
        *[vmem(4, 2, 2, 4, 2, 8, 128) for ch in EARLY_Z],
        dma(CHUNKS, 4), dma(CHUNKS, 4), dma(CHUNKS),
        pltpu.SMEM((128,), jnp.int32), pltpu.VMEM((2, 32), jnp.int32), dma(2),
    ]
    block = pl.BlockSpec(memory_space=pltpu.VMEM)
    hourly, table = pl.pallas_call(
        kernel,
        out_shape=(
            jax.ShapeDtypeStruct((HOURS, 32, 256), jnp.float32),
            jax.ShapeDtypeStruct((8, 128), jnp.float32),
        ),
        in_specs=[pl.BlockSpec(memory_space=pl.ANY)] * 3,
        out_specs=(block, block),
        scratch_shapes=scratch,
        compiler_params=pltpu.CompilerParams(
            collective_id=0, has_side_effects=True, vmem_limit_bytes=52 * 1024 * 1024
        ),
    )(reflectivity.reshape(4, 2, 2, BANDS, 8, 2048), scan_hour, basin_ids.T)
    return pl.pallas_call(
        finish,
        out_shape=(
            jax.ShapeDtypeStruct((HOURS, 32, 256), jnp.float32),
            jax.ShapeDtypeStruct((8, HOURS), jnp.float32),
        ),
        in_specs=[block, block],
        out_specs=(block, block),
        compiler_params=pltpu.CompilerParams(vmem_limit_bytes=8 * 1024 * 1024),
    )(hourly, table)


def solution(mesh):
    placed = (P(("row", "col"), None, None), P(), P("row", "col"))
    return jax.shard_map(
        body,
        mesh=mesh,
        in_specs=placed,
        out_specs=(P(None, "row", "col"), P(("row", "col"), None)),
        check_vma=False,
    )
```

```python
import math

import jax
import jax.numpy as jnp
from jax import lax
from jax.experimental import pallas as pl
from jax.experimental.pallas import tpu as pltpu
from jax.sharding import PartitionSpec as P

MESH = pl.DeviceIdType.MESH
SEG = 128
HOURS = 12
BANDS = 4
CHUNKS = 8
EARLY_Z = (6, 7)
LATE_Z = (3,)
SLOTS = (4, 5)
LOW = 11
LOG2E = 1.0 / math.log(2.0)
SCALE = math.log(10.0) / 16.0 * LOG2E
SHIFT = (math.log(200.0) / 1.6 + math.log(12.0)) * LOG2E


def rain_depth(reflect):
    return jnp.exp2(reflect * SCALE - SHIFT)


def flip(value, mask):
    if mask == 0:
        return value
    if mask == 1:
        return value + 1 - 2 * (value % 2)
    if mask == 2:
        return (value + 2) % 4
    return 3 - value


def masks(parity):
    return (1, 3) if parity == 0 else (3, 1)


def device(x, y, z, c):
    return (z * 4 + (y // 2) * 2 + c, (y % 2) * 4 + x)


def kernel(refl, hours_in, ids_in, out, table_out, *scratch):
    src, got1 = scratch[:2]
    slots_of, gotz, sumz, gotq = (scratch[2 + CHUNKS * i : 2 + CHUNKS * (i + 1)] for i in range(4))
    (
        own_seg, got_seg, seg_hours, got_hours, seg_pack, got_pack, part, part_got, part_sum, part_last, row_sum, row_got,
        load_sem, send1, recv1, sendz, recvz, sendq, recvq, esend1, erecv1, esend2, erecv2, esend3, erecv3,
        bsend1, brecv1, bsend2, brecv2, bsend3, brecv3,
    ) = scratch[2 + CHUNKS * 4 : len(scratch) - 6 - len(EARLY_Z)]
    raw_z = dict(zip(EARLY_Z, scratch[len(scratch) - 6 - len(EARLY_Z) :]))
    sendr, recvr, localr, hours, ids, table_sem = scratch[-6:]
    row, col = lax.axis_index("row"), lax.axis_index("col")
    z, c = row // 4, row % 2
    y, x = ((row // 2) % 2) * 2 + col // 4, col % 4

    barrier = pltpu.get_barrier_semaphore()
    quads = [(0, 1), (1, 0), (1, 1)]
    peers = [device(x, y, z, 1 - c)]
    for mask in (1, 3):
        for ry, rx in quads:
            for core in range(2):
                peers.append(device(flip(x, mask * rx), flip(y, mask * ry), z, core))
    for dz in (1, 2, 3):
        peers.append(device(x, y, (z + dz) % 4, c))
    for peer in peers:
        pl.semaphore_signal(barrier, inc=1, device_id=peer, device_id_type=MESH)

    fetches = [
        pltpu.make_async_copy(hours_in, hours, table_sem.at[0]),
        pltpu.make_async_copy(ids_in, ids, table_sem.at[1]),
    ]

    def load(ch):
        m1, m2 = masks(ch % 2)
        for ry1 in range(2):
            for rx1 in range(2):
                for q in range(4):
                    dy = flip(y, (m1 * ry1) ^ (m2 * (q // 2)))
                    dx = flip(x, (m1 * rx1) ^ (m2 * (q % 2)))
                    lanes = pl.ds(pl.multiple_of(((dy % 2) * 4 + dx) * 256 + (ch % 2) * 128, 128), 128)
                    pltpu.make_async_copy(
                        refl.at[:, dy // 2, :, ch // 2, :, lanes],
                        src.at[ch, ry1, rx1, :, q],
                        load_sem.at[ch],
                    ).start()

    for ch in (0, 1) + EARLY_Z:
        load(ch)
    for copy in fetches:
        copy.start()
    pl.semaphore_wait(barrier, len(peers))

    def clear():
        for ch in range(CHUNKS):
            empty = jnp.zeros(gotz[ch].shape[2:], jnp.float32)
            buf, slots = gotz[ch], SLOTS[ch % 2]

            @pl.loop(0, 4)
            def _(s):
                for k in range(HOURS + LOW):
                    if not LOW <= k < LOW + slots:
                        buf[s, k] = empty


    def copy1(ch, ry1, rx1, tc, sc):
        m1, _ = masks(ch % 2)
        block = raw_z[ch].at[:, ry1, rx1, :, tc] if ch in EARLY_Z else src.at[ch, ry1, rx1, :, :, tc]
        return pltpu.make_async_remote_copy(
            src_ref=block,
            dst_ref=got1.at[ch, ry1, rx1, sc],
            send_sem=send1.at[ch, (ry1 * 2 + rx1) * 2 + tc],
            recv_sem=recv1.at[ch, (ry1 * 2 + rx1) * 2 + sc],
            device_id=device(flip(x, m1 * rx1), flip(y, m1 * ry1), z, tc),
            device_id_type=MESH,
        )

    def step1_copies(ch, mine, which=slice(0, 7)):
        partners = [(ry1, rx1, core) for ry1, rx1 in quads for core in range(2)]
        found = []
        for ry1, rx1, core in (partners + [(0, 0, 1 - c)])[which]:
            found.append(copy1(ch, ry1, rx1, core, c) if mine else copy1(ch, ry1, rx1, c, core))
        return found

    def base_scan(ch, zz):
        return zz * 32 + (y // 2) * 16 if ch % 2 == 0 else zz * 32

    def reduce1(ch):
        m1, _ = masks(ch % 2)
        slots = SLOTS[ch % 2]

        def weights_of(zz):
            first = hours[base_scan(ch, zz)]
            weights = []
            for ry1 in range(2):
                for rx1 in range(2):
                    for core in range(2):
                        yy, xx = flip(y, m1 * ry1), flip(x, m1 * rx1)
                        cc = core if ry1 + rx1 else (c if core == 0 else 1 - c)
                        hour = hours[zz * 32 + (yy // 2) * 16 + cc * 8 + (yy % 2) * 4 + xx]
                        weights.append([jnp.where(hour - first == k, 1.0, 0.0).astype(jnp.float32) for k in range(slots)])
            return weights

        if ch not in EARLY_Z:
            fixed = weights_of(z)

        @pl.loop(0, 4)
        def _(zt):
            weights = weights_of((z - zt + 4) % 4) if ch in EARLY_Z else fixed
            for part_q in (0, 2):
                pair = pl.ds(part_q, 2)
                total = [None] * slots
                n = 0
                for ry1 in range(2):
                    for rx1 in range(2):
                        for core in range(2):
                            if ry1 + rx1:
                                raw = got1[ch, ry1, rx1, core, zt, pair]
                            elif core == 1:
                                raw = got1[ch, 0, 0, 1 - c, zt, pair]
                            elif ch in EARLY_Z:
                                raw = raw_z[ch][zt, 0, 0, pair, c]
                            else:
                                raw = src[ch, 0, 0, zt, pair, c]
                            value = rain_depth(raw)
                            for k in range(slots):
                                term = value * weights[n][k]
                                total[k] = term if total[k] is None else total[k] + term
                            n += 1
                for k in range(slots):
                    if ch in EARLY_Z:
                        gotz[ch][zt, LOW + k, pair] = total[k]
                    elif ch in LATE_Z:
                        slots_of[ch][pair, k, zt] = total[k]
                    else:
                        slots_of[ch][zt, k, pair] = total[k]

    def copyr(ch, dz):
        target_z = (z + dz) % 4
        return pltpu.make_async_remote_copy(
            src_ref=src.at[ch, :, :, target_z],
            dst_ref=raw_z[ch].at[dz],
            send_sem=sendr.at[ch, dz],
            recv_sem=recvr.at[ch, dz],
            device_id=device(x, y, target_z, c),
            device_id_type=MESH,
        )

    def copyr_own(ch):
        return pltpu.make_async_copy(src.at[ch, :, :, z], raw_z[ch].at[0], localr.at[ch])

    def startz(ch, steps=(2, 1, 3)):
        for dz in steps:
            copyr(ch, dz).start()
        if 1 in steps:
            copyr_own(ch).start()

    def copyz(ch, dz):
        target_z = (z + dz) % 4
        block = sumz[ch] if ch in LATE_Z else slots_of[ch]
        return pltpu.make_async_remote_copy(
            src_ref=block.at[target_z],
            dst_ref=gotz[ch].at[dz, pl.ds(LOW, SLOTS[ch % 2])],
            send_sem=sendz.at[ch, dz],
            recv_sem=recvz.at[ch, dz],
            device_id=device(x, y, target_z, c),
            device_id_type=MESH,
        )

    def combinez(ch):
        starts = [LOW - hours[base_scan(ch, (z - dz + 4) % 4)] for dz in range(4)]
        for h in range(HOURS):
            terms = [gotz[ch][dz, starts[dz] + h] for dz in range(4)]
            sumz[ch][:, h] = (terms[0] + terms[1]) + (terms[2] + terms[3])

    def copyq(ch, q):
        _, m2 = masks(ch % 2)
        block = slots_of[ch] if ch in LATE_Z else sumz[ch]
        return pltpu.make_async_remote_copy(
            src_ref=block.at[q],
            dst_ref=gotq[ch].at[q - 1],
            send_sem=sendq.at[ch, q],
            recv_sem=recvq.at[ch, q],
            device_id=device(flip(x, m2 * (q % 2)), flip(y, m2 * (q // 2)), z, c),
            device_id_type=MESH,
        )

    def loaded(*which):
        for ch in which:
            pltpu.make_async_copy(src.at[ch], src.at[ch], load_sem.at[ch]).wait()

    def start1(pair, which=slice(0, 7)):
        for ch in (2 * pair, 2 * pair + 1):
            if ch in EARLY_Z:
                copyr_own(ch).wait()
                for dz in (1, 2, 3):
                    copyr(ch, dz).wait_recv()
        for one, two in zip(step1_copies(2 * pair, True, which), step1_copies(2 * pair + 1, True, which)):
            one.start()
            two.start()

    def send_z(ch, block):
        for dz in (1, 3, 2):
            copyz(ch, dz).start()
        for k in range(SLOTS[ch % 2]):
            gotz[ch][0, LOW + k] = block[z, k]

    def send_q(ch):
        for q in (3, 1, 2):
            copyq(ch, q).start()

    def first(*which):
        for ch in which:
            for copy in step1_copies(ch, False):
                copy.wait_recv()
            reduce1(ch)
            if ch in EARLY_Z:
                combinez(ch)
            if ch in EARLY_Z + LATE_Z:
                send_q(ch)
            else:
                send_z(ch, slots_of[ch])

    def second(*which):
        for ch in which:
            if ch in LATE_Z:
                for q in (1, 2, 3):
                    copyq(ch, q).wait_recv()
                for zt in range(4):
                    for k in range(SLOTS[ch % 2]):
                        sumz[ch][zt, k] = (slots_of[ch][0, k, zt] + gotq[ch][0, k, zt]) + (
                            gotq[ch][1, k, zt] + gotq[ch][2, k, zt]
                        )
                send_z(ch, sumz[ch])
            else:
                for dz in (1, 2, 3):
                    copyz(ch, dz).wait_recv()
                combinez(ch)
                send_q(ch)

    def third(*which):
        for ch in which:
            band = slice(ch // 2 * 8, ch // 2 * 8 + 8)
            half = slice(ch % 2 * 128, ch % 2 * 128 + 128)
            if ch in LATE_Z:
                for dz in (1, 2, 3):
                    copyz(ch, dz).wait_recv()
                starts = [LOW - hours[base_scan(ch, (z - dz + 4) % 4)] for dz in range(4)]
            else:
                for q in (1, 2, 3):
                    copyq(ch, q).wait_recv()
            for h in range(HOURS):
                if ch in LATE_Z:
                    terms = [gotz[ch][dz, starts[dz] + h] for dz in range(4)]
                else:
                    terms = [sumz[ch][0, h]] + [gotq[ch][n, h] for n in range(3)]
                out[h, band, half] = (terms[0] + terms[1]) + (terms[2] + terms[3])

    lane = lax.broadcasted_iota(jnp.int32, (8, 128), 1)

    def own_segments():
        def one_z(zt, totals):
            totals = list(totals)
            here = lane - zt * 32
            for q in range(4):
                for ch in range(CHUNKS):
                    spot = here == q * 8 + ch
                    for n in range(8):
                        ey1, ex1, core = n // 4, (n // 2) % 2, n % 2
                        if ch % 2 == 0:
                            raw = src[ch, ey1, ex1, zt, q, core]
                        else:
                            raw = src[ch, q // 2, q % 2, zt, ey1 * 2 + ex1, core]
                        total = jnp.sum(rain_depth(raw), axis=1, keepdims=True)
                        totals[n] = jnp.where(spot, total, totals[n])
            return tuple(totals)

        totals = lax.fori_loop(0, 4, one_z, tuple(jnp.zeros((8, 128), jnp.float32) for _ in range(8)))
        for n in range(8):
            own_seg[n // 4, (n // 2) % 2, n % 2] = totals[n]

    def ecopy1(ry1, rx1, tc, sc):
        n = (ry1 * 2 + rx1) * 2
        return pltpu.make_async_remote_copy(
            src_ref=own_seg.at[ry1, rx1, tc],
            dst_ref=got_seg.at[ry1, rx1, sc],
            send_sem=esend1.at[n + tc],
            recv_sem=erecv1.at[n + sc],
            device_id=device(flip(x, rx1), flip(y, ry1), z, tc),
            device_id_type=MESH,
        )

    def ecopy2(dz):
        return pltpu.make_async_remote_copy(
            src_ref=seg_hours.at[dz],
            dst_ref=got_hours.at[dz - 1],
            send_sem=esend2.at[dz],
            recv_sem=erecv2.at[dz],
            device_id=device(x, y, (z + dz) % 4, c),
            device_id_type=MESH,
        )

    def ecopy3(q):
        return pltpu.make_async_remote_copy(
            src_ref=seg_pack,
            dst_ref=got_pack.at[q - 1],
            send_sem=esend3.at[q],
            recv_sem=erecv3.at[q],
            device_id=device(flip(x, 3 * (q % 2)), flip(y, 3 * (q // 2)), z, c),
            device_id_type=MESH,
        )

    def quad_out(copy):
        found = [copy(ry1, rx1, core, c) for ry1, rx1 in quads for core in range(2)]
        return found + [copy(0, 0, 1 - c, c)]

    def quad_in(copy):
        found = [copy(ry1, rx1, c, core) for ry1, rx1 in quads for core in range(2)]
        return found + [copy(0, 0, c, 1 - c)]

    def segments1():
        loaded(*[ch for ch in range(2, CHUNKS) if ch not in EARLY_Z])
        own_segments()
        for copy in quad_out(ecopy1):
            copy.start()

    def segments2():
        for copy in quad_in(ecopy1):
            copy.wait_recv()
        totals = [None] * HOURS
        for ry1 in range(2):
            for rx1 in range(2):
                for core in range(2):
                    yy, xx = flip(y, ry1), flip(x, rx1)
                    if ry1 + rx1:
                        cc, value = core, got_seg[ry1, rx1, core]
                    elif core == 0:
                        cc, value = c, own_seg[0, 0, c]
                    else:
                        cc, value = 1 - c, got_seg[0, 0, 1 - c]
                    hour = hours[z * 32 + (yy // 2) * 16 + cc * 8 + (yy % 2) * 4 + xx]
                    for h in range(HOURS):
                        term = value * jnp.where(hour == h, 1.0, 0.0).astype(jnp.float32)
                        totals[h] = term if totals[h] is None else totals[h] + term
        for dz in (2, 1, 3, 0):
            for k in range(HOURS // 4):
                packed = jnp.zeros((8, 128), jnp.float32)
                for h in range(4 * k, 4 * k + 4):
                    value = jnp.where(lane // 32 == (z + dz) % 4, totals[h], 0.0)
                    value = value + pltpu.roll(value, 64, 1)
                    value = value + pltpu.roll(value, 32, 1)
                    packed = jnp.where(lane // 32 == h % 4, value, packed)
                seg_hours[dz, k] = packed
        for dz in (2, 1, 3):
            ecopy2(dz).start()

    def segments3():
        for dz in (1, 2, 3):
            ecopy2(dz).wait_recv()
        for k in range(HOURS // 4):
            seg_pack[k] = (seg_hours[0, k] + got_hours[0, k]) + (got_hours[1, k] + got_hours[2, k])
        for q in (3, 1, 2):
            ecopy3(q).start()

    def shares():
        for q in (1, 2, 3):
            ecopy3(q).wait_recv()
        table = []
        for k in range(HOURS // 4):
            value = seg_pack[k]
            for q in (1, 2, 3):
                value = value + pltpu.roll(got_pack[q - 1, k], 128 - 8 * q, 1)
            table.append(value)
        tile_rows = out.shape[1]
        wide = lax.broadcasted_iota(jnp.int32, (tile_rows, 128), 1)
        rank = lax.broadcasted_iota(jnp.int32, (128, tile_rows), 0)
        oz, orx2, ory2 = rank % 4, (rank // 4) % 2, (rank // 8) % 2
        oc, orx1, ory1 = (rank // 16) % 2, (rank // 32) % 2, rank // 64

        def flip_each(value, bit, mask):
            return jnp.where(bit == 1, flip(value, mask), value)

        ox = flip_each(flip_each(jnp.full_like(rank, x), orx1, 1), orx2, 3)
        oy = flip_each(flip_each(jnp.full_like(rank, y), ory1, 1), ory2, 3)
        owner = (oz * 4 + (oy // 2) * 2 + oc) * 8 + (oy % 2) * 4 + ox
        square = (tile_rows, tile_rows)
        diagonal = lax.broadcasted_iota(jnp.int32, square, 0) == lax.broadcasted_iota(jnp.int32, square, 1)
        share = jnp.zeros((128, 128), jnp.float32)
        for g in range(2):
            bands = []
            for j in range(BANDS):
                value = jnp.where(lane % 16 == HOURS, float(SEG), 0.0)
                for h in range(HOURS):
                    at = (h % 4) * 32 + j * 2 + g
                    value = jnp.where(lane % 16 == h, table[h // 4][:, at : at + 1], value)
                bands.append(value)
            value = jnp.concatenate(bands, axis=0)
            names = ids[g : g + 1, :]
            place = (names % 8).astype(jnp.float32)
            place = jnp.sum(jnp.where(diagonal, place, 0.0), axis=1, keepdims=True)
            value = jnp.where((wide // 16).astype(jnp.float32) == place, value, 0.0)
            chosen = jnp.where(owner == names // 8, 1.0, 0.0)
            share = share + jnp.dot(
                chosen, value, precision=lax.Precision.HIGHEST, preferred_element_type=jnp.float32
            )
        part[...] = share.reshape(8, 16, 128)
        for copy in quad_out(bcopy1):
            copy.start()

    def bcopy1(ry1, rx1, tc, sc):
        n = (ry1 * 2 + rx1) * 2
        return pltpu.make_async_remote_copy(
            src_ref=part.at[n + tc],
            dst_ref=part_got.at[n + sc],
            send_sem=bsend1.at[n + tc],
            recv_sem=brecv1.at[n + sc],
            device_id=device(flip(x, rx1), flip(y, ry1), z, tc),
            device_id_type=MESH,
        )

    def bcopy2(q):
        return pltpu.make_async_remote_copy(
            src_ref=part_sum,
            dst_ref=part_last.at[q - 1],
            send_sem=bsend2.at[q],
            recv_sem=brecv2.at[q],
            device_id=device(flip(x, 3 * (q % 2)), flip(y, 3 * (q // 2)), z, c),
            device_id_type=MESH,
        )

    def bcopy3(dz):
        return pltpu.make_async_remote_copy(
            src_ref=row_sum,
            dst_ref=row_got.at[dz - 1],
            send_sem=bsend3.at[dz],
            recv_sem=brecv3.at[dz],
            device_id=device(x, y, (z + dz) % 4, c),
            device_id_type=MESH,
        )

    def shares2():
        for copy in quad_in(bcopy1):
            copy.wait_recv()
        summed = part[c] + part_got[1 - c]
        for ry1, rx1 in quads:
            for core in range(2):
                summed = summed + part_got[(ry1 * 2 + rx1) * 2 + core]
        part_sum[...] = summed
        for q in (3, 1, 2):
            bcopy2(q).start()

    def shares3():
        for q in (1, 2, 3):
            bcopy2(q).wait_recv()
        row_sum[...] = jnp.zeros((8, 128), jnp.float32)
        row_sum[0:4] = (part_sum[0:4] + part_last[0, 4:8]) + (part_last[1, 8:12] + part_last[2, 12:16])
        for dz in (2, 1, 3):
            bcopy3(dz).start()

    def shares4():
        final = row_sum[pl.ds(z, 1), :]
        for dz in (1, 2, 3):
            bcopy3(dz).wait_recv()
        for dz in (1, 2, 3):
            final = final + row_got[dz - 1, pl.ds(z, 1), :]
        row8 = lax.broadcasted_iota(jnp.int32, (8, 128), 0)
        spread = jnp.where(lane // 16 == row8, jnp.broadcast_to(final, (8, 128)), 0.0)
        lane_in = lax.broadcasted_iota(jnp.int32, (128, 128), 0)
        lane_out = lax.broadcasted_iota(jnp.int32, (128, 128), 1)
        pick = jnp.where(lane_in % 16 == lane_out, 1.0, 0.0)
        table_out[...] = jnp.dot(
            spread, pick, precision=lax.Precision.HIGHEST, preferred_element_type=jnp.float32
        )

    def sent():
        for ch in range(CHUNKS):
            for copy in step1_copies(ch, True):
                copy.wait_send()
            for dz in (1, 2, 3):
                (copyr if ch in EARLY_Z else copyz)(ch, dz).wait_send()
        for copy in quad_out(ecopy1) + quad_out(bcopy1):
            copy.wait_send()
        for n in (1, 2, 3):
            for small in (ecopy2, ecopy3, bcopy2, bcopy3):
                small(n).wait_send()

    loaded(0, 1)
    start1(0, slice(0, 4))
    for ch in range(2, CHUNKS):
        if ch not in EARLY_Z:
            load(ch)
    loaded(*EARLY_Z)
    startz(6)
    startz(7, (2,))
    segments1()
    for copy in fetches:
        copy.wait()
    start1(0, slice(4, 7))
    start1(1)
    clear()
    segments2()
    startz(7, (1, 3))
    first(0)
    first(1)
    segments3()
    start1(2)
    shares()
    start1(3)
    first(3)
    first(2)
    second(0)
    first(4)
    first(5)
    shares2()
    second(1)
    second(2)
    second(4)
    first(7)
    first(6)
    third(0)
    shares3()
    second(3)
    second(5)
    third(2)
    shares4()
    third(1)
    third(4)
    sent()
    third(3)
    third(7)
    third(6)
    third(5)

    for ch in range(CHUNKS):
        for q in (1, 2, 3):
            copyq(ch, q).wait_send()


def finish(hourly, table, out, depth):
    out[...] = hourly[...]
    depth[...] = (table[...] / table[:, HOURS : HOURS + 1])[:, :HOURS]


def body(reflectivity, scan_hour, basin_ids):
    def vmem(*shape):
        return pltpu.VMEM(shape, jnp.float32)

    def dma(*shape):
        return pltpu.SemaphoreType.DMA(shape)

    chunks = range(CHUNKS)
    scratch = [
        vmem(CHUNKS, 2, 2, 4, 4, 2, 8, 128),
        vmem(CHUNKS, 2, 2, 2, 4, 4, 8, 128),
        *[vmem(4, 1 if ch in EARLY_Z else SLOTS[ch % 2], 4, 8, 128) for ch in chunks],
        *[vmem(4, HOURS + LOW, *((8, 128) if ch in LATE_Z else (4, 8, 128))) for ch in chunks],
        *[vmem(4, SLOTS[1] if ch in LATE_Z else HOURS, 8, 128) for ch in chunks],
        *[vmem(3, *((SLOTS[1], 4) if ch in LATE_Z else (HOURS,)), 8, 128) for ch in chunks],
        vmem(2, 2, 2, 8, 128), vmem(2, 2, 2, 8, 128), vmem(4, HOURS // 4, 8, 128), vmem(3, HOURS // 4, 8, 128),
        vmem(HOURS // 4, 8, 128), vmem(3, HOURS // 4, 8, 128),
        vmem(8, 16, 128), vmem(8, 16, 128), vmem(16, 128), vmem(3, 16, 128), vmem(8, 128), vmem(3, 8, 128),
        dma(CHUNKS), dma(CHUNKS, 8), dma(CHUNKS, 8), dma(CHUNKS, 4), dma(CHUNKS, 4), dma(CHUNKS, 4), dma(CHUNKS, 4),
        dma(8), dma(8), dma(4), dma(4), dma(4), dma(4), dma(8), dma(8), dma(4), dma(4), dma(4), dma(4),
        *[vmem(4, 2, 2, 4, 2, 8, 128) for ch in EARLY_Z],
        dma(CHUNKS, 4), dma(CHUNKS, 4), dma(CHUNKS),
        pltpu.SMEM((128,), jnp.int32), pltpu.VMEM((2, 32), jnp.int32), dma(2),
    ]
    block = pl.BlockSpec(memory_space=pltpu.VMEM)
    hourly, table = pl.pallas_call(
        kernel,
        out_shape=(
            jax.ShapeDtypeStruct((HOURS, 32, 256), jnp.float32),
            jax.ShapeDtypeStruct((8, 128), jnp.float32),
        ),
        in_specs=[pl.BlockSpec(memory_space=pl.ANY)] * 3,
        out_specs=(block, block),
        scratch_shapes=scratch,
        compiler_params=pltpu.CompilerParams(
            collective_id=0, has_side_effects=True, vmem_limit_bytes=52 * 1024 * 1024
        ),
    )(reflectivity.reshape(4, 2, 2, BANDS, 8, 2048), scan_hour, basin_ids.T)
    return pl.pallas_call(
        finish,
        out_shape=(
            jax.ShapeDtypeStruct((HOURS, 32, 256), jnp.float32),
            jax.ShapeDtypeStruct((8, HOURS), jnp.float32),
        ),
        in_specs=[block, block],
        out_specs=(block, block),
        compiler_params=pltpu.CompilerParams(vmem_limit_bytes=8 * 1024 * 1024),
    )(hourly, table)


def solution(mesh):
    placed = (P(("row", "col"), None, None), P(), P("row", "col"))
    return jax.shard_map(
        body,
        mesh=mesh,
        in_specs=placed,
        out_specs=(P(None, "row", "col"), P(("row", "col"), None)),
        check_vma=False,
    )
```

```python
import math

import jax
import jax.numpy as jnp
from jax import lax
from jax.experimental import pallas as pl
from jax.experimental.pallas import tpu as pltpu
from jax.sharding import PartitionSpec as P

MESH = pl.DeviceIdType.MESH
SEG = 128
HOURS = 12
BANDS = 4
CHUNKS = 8
EARLY_Z = (6, 7)
LATE_Z = (3,)
SLOTS = (4, 5)
LOW = 11
LOG2E = 1.0 / math.log(2.0)
SCALE = math.log(10.0) / 16.0 * LOG2E
SHIFT = (math.log(200.0) / 1.6 + math.log(12.0)) * LOG2E


def rain_depth(reflect):
    return jnp.exp2(reflect * SCALE - SHIFT)


def flip(value, mask):
    if mask == 0:
        return value
    if mask == 1:
        return value + 1 - 2 * (value % 2)
    if mask == 2:
        return (value + 2) % 4
    return 3 - value


def masks(parity):
    return (1, 3) if parity == 0 else (3, 1)


def device(x, y, z, c):
    return (z * 4 + (y // 2) * 2 + c, (y % 2) * 4 + x)


def kernel(refl, hours_in, ids_in, out, table_out, *scratch):
    src, got1 = scratch[:2]
    slots_of, gotz, sumz, gotq = (scratch[2 + CHUNKS * i : 2 + CHUNKS * (i + 1)] for i in range(4))
    (
        own_seg, got_seg, seg_hours, got_hours, seg_pack, got_pack, part, part_got, part_sum, part_last, row_sum, row_got,
        load_sem, send1, recv1, sendz, recvz, sendq, recvq, esend1, erecv1, esend2, erecv2, esend3, erecv3,
        bsend1, brecv1, bsend2, brecv2, bsend3, brecv3,
    ) = scratch[2 + CHUNKS * 4 : len(scratch) - 6 - len(EARLY_Z)]
    raw_z = dict(zip(EARLY_Z, scratch[len(scratch) - 6 - len(EARLY_Z) :]))
    sendr, recvr, localr, hours, ids, table_sem = scratch[-6:]
    row, col = lax.axis_index("row"), lax.axis_index("col")
    z, c = row // 4, row % 2
    y, x = ((row // 2) % 2) * 2 + col // 4, col % 4

    barrier = pltpu.get_barrier_semaphore()
    quads = [(0, 1), (1, 0), (1, 1)]
    peers = [device(x, y, z, 1 - c)]
    for mask in (1, 3):
        for ry, rx in quads:
            for core in range(2):
                peers.append(device(flip(x, mask * rx), flip(y, mask * ry), z, core))
    for dz in (1, 2, 3):
        peers.append(device(x, y, (z + dz) % 4, c))
    for peer in peers:
        pl.semaphore_signal(barrier, inc=1, device_id=peer, device_id_type=MESH)

    fetches = [
        pltpu.make_async_copy(hours_in, hours, table_sem.at[0]),
        pltpu.make_async_copy(ids_in, ids, table_sem.at[1]),
    ]

    def load(ch):
        m1, m2 = masks(ch % 2)
        for ry1 in range(2):
            for rx1 in range(2):
                for q in range(4):
                    dy = flip(y, (m1 * ry1) ^ (m2 * (q // 2)))
                    dx = flip(x, (m1 * rx1) ^ (m2 * (q % 2)))
                    lanes = pl.ds(pl.multiple_of(((dy % 2) * 4 + dx) * 256 + (ch % 2) * 128, 128), 128)
                    pltpu.make_async_copy(
                        refl.at[:, dy // 2, :, ch // 2, :, lanes],
                        src.at[ch, ry1, rx1, :, q],
                        load_sem.at[ch],
                    ).start()

    for ch in (0, 1) + EARLY_Z:
        load(ch)
    for copy in fetches:
        copy.start()
    pl.semaphore_wait(barrier, len(peers))

    def clear():
        for ch in range(CHUNKS):
            empty = jnp.zeros(gotz[ch].shape[2:], jnp.float32)
            buf, slots = gotz[ch], SLOTS[ch % 2]

            @pl.loop(0, 4)
            def _(s):
                for k in range(HOURS + LOW):
                    if not LOW <= k < LOW + slots:
                        buf[s, k] = empty


    def copy1(ch, ry1, rx1, tc, sc):
        m1, _ = masks(ch % 2)
        block = raw_z[ch].at[:, ry1, rx1, :, tc] if ch in EARLY_Z else src.at[ch, ry1, rx1, :, :, tc]
        return pltpu.make_async_remote_copy(
            src_ref=block,
            dst_ref=got1.at[ch, ry1, rx1, sc],
            send_sem=send1.at[ch, (ry1 * 2 + rx1) * 2 + tc],
            recv_sem=recv1.at[ch, (ry1 * 2 + rx1) * 2 + sc],
            device_id=device(flip(x, m1 * rx1), flip(y, m1 * ry1), z, tc),
            device_id_type=MESH,
        )

    def step1_copies(ch, mine, which=slice(0, 7)):
        partners = [(ry1, rx1, core) for ry1, rx1 in quads for core in range(2)]
        found = []
        for ry1, rx1, core in (partners + [(0, 0, 1 - c)])[which]:
            found.append(copy1(ch, ry1, rx1, core, c) if mine else copy1(ch, ry1, rx1, c, core))
        return found

    def base_scan(ch, zz):
        return zz * 32 + (y // 2) * 16 if ch % 2 == 0 else zz * 32

    def reduce1(ch):
        m1, _ = masks(ch % 2)
        slots = SLOTS[ch % 2]

        def weights_of(zz):
            first = hours[base_scan(ch, zz)]
            weights = []
            for ry1 in range(2):
                for rx1 in range(2):
                    for core in range(2):
                        yy, xx = flip(y, m1 * ry1), flip(x, m1 * rx1)
                        cc = core if ry1 + rx1 else (c if core == 0 else 1 - c)
                        hour = hours[zz * 32 + (yy // 2) * 16 + cc * 8 + (yy % 2) * 4 + xx]
                        weights.append([jnp.where(hour - first == k, 1.0, 0.0).astype(jnp.float32) for k in range(slots)])
            return weights

        if ch not in EARLY_Z:
            fixed = weights_of(z)

        @pl.loop(0, 4)
        def _(zt):
            weights = weights_of((z - zt + 4) % 4) if ch in EARLY_Z else fixed
            for part_q in (0, 2):
                pair = pl.ds(part_q, 2)
                total = [None] * slots
                n = 0
                for ry1 in range(2):
                    for rx1 in range(2):
                        for core in range(2):
                            if ry1 + rx1:
                                raw = got1[ch, ry1, rx1, core, zt, pair]
                            elif core == 1:
                                raw = got1[ch, 0, 0, 1 - c, zt, pair]
                            elif ch in EARLY_Z:
                                raw = raw_z[ch][zt, 0, 0, pair, c]
                            else:
                                raw = src[ch, 0, 0, zt, pair, c]
                            value = rain_depth(raw)
                            for k in range(slots):
                                term = value * weights[n][k]
                                total[k] = term if total[k] is None else total[k] + term
                            n += 1
                for k in range(slots):
                    if ch in EARLY_Z:
                        gotz[ch][zt, LOW + k, pair] = total[k]
                    elif ch in LATE_Z:
                        slots_of[ch][pair, k, zt] = total[k]
                    else:
                        slots_of[ch][zt, k, pair] = total[k]

    def copyr(ch, dz):
        target_z = (z + dz) % 4
        return pltpu.make_async_remote_copy(
            src_ref=src.at[ch, :, :, target_z],
            dst_ref=raw_z[ch].at[dz],
            send_sem=sendr.at[ch, dz],
            recv_sem=recvr.at[ch, dz],
            device_id=device(x, y, target_z, c),
            device_id_type=MESH,
        )

    def copyr_own(ch):
        return pltpu.make_async_copy(src.at[ch, :, :, z], raw_z[ch].at[0], localr.at[ch])

    def startz(ch, steps=(2, 1, 3)):
        for dz in steps:
            copyr(ch, dz).start()
        if 1 in steps:
            copyr_own(ch).start()

    def copyz(ch, dz):
        target_z = (z + dz) % 4
        block = sumz[ch] if ch in LATE_Z else slots_of[ch]
        return pltpu.make_async_remote_copy(
            src_ref=block.at[target_z],
            dst_ref=gotz[ch].at[dz, pl.ds(LOW, SLOTS[ch % 2])],
            send_sem=sendz.at[ch, dz],
            recv_sem=recvz.at[ch, dz],
            device_id=device(x, y, target_z, c),
            device_id_type=MESH,
        )

    def combinez(ch):
        starts = [LOW - hours[base_scan(ch, (z - dz + 4) % 4)] for dz in range(4)]
        for h in range(HOURS):
            terms = [gotz[ch][dz, starts[dz] + h] for dz in range(4)]
            sumz[ch][:, h] = (terms[0] + terms[1]) + (terms[2] + terms[3])

    def copyq(ch, q):
        _, m2 = masks(ch % 2)
        block = slots_of[ch] if ch in LATE_Z else sumz[ch]
        return pltpu.make_async_remote_copy(
            src_ref=block.at[q],
            dst_ref=gotq[ch].at[q - 1],
            send_sem=sendq.at[ch, q],
            recv_sem=recvq.at[ch, q],
            device_id=device(flip(x, m2 * (q % 2)), flip(y, m2 * (q // 2)), z, c),
            device_id_type=MESH,
        )

    def loaded(*which):
        for ch in which:
            pltpu.make_async_copy(src.at[ch], src.at[ch], load_sem.at[ch]).wait()

    def start1(pair, which=slice(0, 7)):
        for ch in (2 * pair, 2 * pair + 1):
            if ch in EARLY_Z:
                copyr_own(ch).wait()
                for dz in (1, 2, 3):
                    copyr(ch, dz).wait_recv()
        for one, two in zip(step1_copies(2 * pair, True, which), step1_copies(2 * pair + 1, True, which)):
            one.start()
            two.start()

    def send_z(ch, block):
        for dz in (1, 3, 2):
            copyz(ch, dz).start()
        for k in range(SLOTS[ch % 2]):
            gotz[ch][0, LOW + k] = block[z, k]

    def send_q(ch):
        for q in (3, 1, 2):
            copyq(ch, q).start()

    def first(*which):
        for ch in which:
            for copy in step1_copies(ch, False):
                copy.wait_recv()
            reduce1(ch)
            if ch in EARLY_Z:
                combinez(ch)
            if ch in EARLY_Z + LATE_Z:
                send_q(ch)
            else:
                send_z(ch, slots_of[ch])

    def second(*which):
        for ch in which:
            if ch in LATE_Z:
                for q in (1, 2, 3):
                    copyq(ch, q).wait_recv()
                for zt in range(4):
                    for k in range(SLOTS[ch % 2]):
                        sumz[ch][zt, k] = (slots_of[ch][0, k, zt] + gotq[ch][0, k, zt]) + (
                            gotq[ch][1, k, zt] + gotq[ch][2, k, zt]
                        )
                send_z(ch, sumz[ch])
            else:
                for dz in (1, 2, 3):
                    copyz(ch, dz).wait_recv()
                combinez(ch)
                send_q(ch)

    def third(*which):
        for ch in which:
            band = slice(ch // 2 * 8, ch // 2 * 8 + 8)
            half = slice(ch % 2 * 128, ch % 2 * 128 + 128)
            if ch in LATE_Z:
                for dz in (1, 2, 3):
                    copyz(ch, dz).wait_recv()
                starts = [LOW - hours[base_scan(ch, (z - dz + 4) % 4)] for dz in range(4)]
            else:
                for q in (1, 2, 3):
                    copyq(ch, q).wait_recv()
            for h in range(HOURS):
                if ch in LATE_Z:
                    terms = [gotz[ch][dz, starts[dz] + h] for dz in range(4)]
                else:
                    terms = [sumz[ch][0, h]] + [gotq[ch][n, h] for n in range(3)]
                out[h, band, half] = (terms[0] + terms[1]) + (terms[2] + terms[3])

    lane = lax.broadcasted_iota(jnp.int32, (8, 128), 1)

    def own_segments():
        def one_z(zt, totals):
            totals = list(totals)
            here = lane - zt * 32
            for q in range(4):
                for ch in range(CHUNKS):
                    spot = here == q * 8 + ch
                    for n in range(8):
                        ey1, ex1, core = n // 4, (n // 2) % 2, n % 2
                        if ch % 2 == 0:
                            raw = src[ch, ey1, ex1, zt, q, core]
                        else:
                            raw = src[ch, q // 2, q % 2, zt, ey1 * 2 + ex1, core]
                        total = jnp.sum(rain_depth(raw), axis=1, keepdims=True)
                        totals[n] = jnp.where(spot, total, totals[n])
            return tuple(totals)

        totals = lax.fori_loop(0, 4, one_z, tuple(jnp.zeros((8, 128), jnp.float32) for _ in range(8)))
        for n in range(8):
            own_seg[n // 4, (n // 2) % 2, n % 2] = totals[n]

    def ecopy1(ry1, rx1, tc, sc):
        n = (ry1 * 2 + rx1) * 2
        return pltpu.make_async_remote_copy(
            src_ref=own_seg.at[ry1, rx1, tc],
            dst_ref=got_seg.at[ry1, rx1, sc],
            send_sem=esend1.at[n + tc],
            recv_sem=erecv1.at[n + sc],
            device_id=device(flip(x, rx1), flip(y, ry1), z, tc),
            device_id_type=MESH,
        )

    def ecopy2(dz):
        return pltpu.make_async_remote_copy(
            src_ref=seg_hours.at[dz],
            dst_ref=got_hours.at[dz - 1],
            send_sem=esend2.at[dz],
            recv_sem=erecv2.at[dz],
            device_id=device(x, y, (z + dz) % 4, c),
            device_id_type=MESH,
        )

    def ecopy3(q):
        return pltpu.make_async_remote_copy(
            src_ref=seg_pack,
            dst_ref=got_pack.at[q - 1],
            send_sem=esend3.at[q],
            recv_sem=erecv3.at[q],
            device_id=device(flip(x, 3 * (q % 2)), flip(y, 3 * (q // 2)), z, c),
            device_id_type=MESH,
        )

    def quad_out(copy):
        found = [copy(ry1, rx1, core, c) for ry1, rx1 in quads for core in range(2)]
        return found + [copy(0, 0, 1 - c, c)]

    def quad_in(copy):
        found = [copy(ry1, rx1, c, core) for ry1, rx1 in quads for core in range(2)]
        return found + [copy(0, 0, c, 1 - c)]

    def segments1():
        loaded(*[ch for ch in range(2, CHUNKS) if ch not in EARLY_Z])
        own_segments()
        for copy in quad_out(ecopy1):
            copy.start()

    def segments2():
        for copy in quad_in(ecopy1):
            copy.wait_recv()
        totals = [None] * HOURS
        for ry1 in range(2):
            for rx1 in range(2):
                for core in range(2):
                    yy, xx = flip(y, ry1), flip(x, rx1)
                    if ry1 + rx1:
                        cc, value = core, got_seg[ry1, rx1, core]
                    elif core == 0:
                        cc, value = c, own_seg[0, 0, c]
                    else:
                        cc, value = 1 - c, got_seg[0, 0, 1 - c]
                    hour = hours[z * 32 + (yy // 2) * 16 + cc * 8 + (yy % 2) * 4 + xx]
                    for h in range(HOURS):
                        term = value * jnp.where(hour == h, 1.0, 0.0).astype(jnp.float32)
                        totals[h] = term if totals[h] is None else totals[h] + term
        for dz in (2, 1, 3, 0):
            for k in range(HOURS // 4):
                packed = jnp.zeros((8, 128), jnp.float32)
                for h in range(4 * k, 4 * k + 4):
                    value = jnp.where(lane // 32 == (z + dz) % 4, totals[h], 0.0)
                    value = value + pltpu.roll(value, 64, 1)
                    value = value + pltpu.roll(value, 32, 1)
                    packed = jnp.where(lane // 32 == h % 4, value, packed)
                seg_hours[dz, k] = packed
        for dz in (2, 1, 3):
            ecopy2(dz).start()

    def segments3():
        for dz in (1, 2, 3):
            ecopy2(dz).wait_recv()
        for k in range(HOURS // 4):
            seg_pack[k] = (seg_hours[0, k] + got_hours[0, k]) + (got_hours[1, k] + got_hours[2, k])
        for q in (3, 1, 2):
            ecopy3(q).start()

    def shares():
        for q in (1, 2, 3):
            ecopy3(q).wait_recv()
        table = []
        for k in range(HOURS // 4):
            value = seg_pack[k]
            for q in (1, 2, 3):
                value = value + pltpu.roll(got_pack[q - 1, k], 128 - 8 * q, 1)
            table.append(value)
        tile_rows = out.shape[1]
        wide = lax.broadcasted_iota(jnp.int32, (tile_rows, 128), 1)
        rank = lax.broadcasted_iota(jnp.int32, (128, tile_rows), 0)
        oz, orx2, ory2 = rank % 4, (rank // 4) % 2, (rank // 8) % 2
        oc, orx1, ory1 = (rank // 16) % 2, (rank // 32) % 2, rank // 64

        def flip_each(value, bit, mask):
            return jnp.where(bit == 1, flip(value, mask), value)

        ox = flip_each(flip_each(jnp.full_like(rank, x), orx1, 1), orx2, 3)
        oy = flip_each(flip_each(jnp.full_like(rank, y), ory1, 1), ory2, 3)
        owner = (oz * 4 + (oy // 2) * 2 + oc) * 8 + (oy % 2) * 4 + ox
        square = (tile_rows, tile_rows)
        diagonal = lax.broadcasted_iota(jnp.int32, square, 0) == lax.broadcasted_iota(jnp.int32, square, 1)
        share = jnp.zeros((128, 128), jnp.float32)
        for g in range(2):
            bands = []
            for j in range(BANDS):
                value = jnp.where(lane % 16 == HOURS, float(SEG), 0.0)
                for h in range(HOURS):
                    at = (h % 4) * 32 + j * 2 + g
                    value = jnp.where(lane % 16 == h, table[h // 4][:, at : at + 1], value)
                bands.append(value)
            value = jnp.concatenate(bands, axis=0)
            names = ids[g : g + 1, :]
            place = (names % 8).astype(jnp.float32)
            place = jnp.sum(jnp.where(diagonal, place, 0.0), axis=1, keepdims=True)
            value = jnp.where((wide // 16).astype(jnp.float32) == place, value, 0.0)
            chosen = jnp.where(owner == names // 8, 1.0, 0.0)
            share = share + jnp.dot(
                chosen, value, precision=lax.Precision.HIGHEST, preferred_element_type=jnp.float32
            )
        part[...] = share.reshape(8, 16, 128)
        for copy in quad_out(bcopy1):
            copy.start()

    def bcopy1(ry1, rx1, tc, sc):
        n = (ry1 * 2 + rx1) * 2
        return pltpu.make_async_remote_copy(
            src_ref=part.at[n + tc],
            dst_ref=part_got.at[n + sc],
            send_sem=bsend1.at[n + tc],
            recv_sem=brecv1.at[n + sc],
            device_id=device(flip(x, rx1), flip(y, ry1), z, tc),
            device_id_type=MESH,
        )

    def bcopy2(q):
        return pltpu.make_async_remote_copy(
            src_ref=part_sum,
            dst_ref=part_last.at[q - 1],
            send_sem=bsend2.at[q],
            recv_sem=brecv2.at[q],
            device_id=device(flip(x, 3 * (q % 2)), flip(y, 3 * (q // 2)), z, c),
            device_id_type=MESH,
        )

    def bcopy3(dz):
        return pltpu.make_async_remote_copy(
            src_ref=row_sum,
            dst_ref=row_got.at[dz - 1],
            send_sem=bsend3.at[dz],
            recv_sem=brecv3.at[dz],
            device_id=device(x, y, (z + dz) % 4, c),
            device_id_type=MESH,
        )

    def shares2():
        for copy in quad_in(bcopy1):
            copy.wait_recv()
        summed = part[c] + part_got[1 - c]
        for ry1, rx1 in quads:
            for core in range(2):
                summed = summed + part_got[(ry1 * 2 + rx1) * 2 + core]
        part_sum[...] = summed
        for q in (3, 1, 2):
            bcopy2(q).start()

    def shares3():
        for q in (1, 2, 3):
            bcopy2(q).wait_recv()
        row_sum[...] = jnp.zeros((8, 128), jnp.float32)
        row_sum[0:4] = (part_sum[0:4] + part_last[0, 4:8]) + (part_last[1, 8:12] + part_last[2, 12:16])
        for dz in (2, 1, 3):
            bcopy3(dz).start()

    def shares4():
        final = row_sum[pl.ds(z, 1), :]
        for dz in (1, 2, 3):
            bcopy3(dz).wait_recv()
        for dz in (1, 2, 3):
            final = final + row_got[dz - 1, pl.ds(z, 1), :]
        row8 = lax.broadcasted_iota(jnp.int32, (8, 128), 0)
        spread = jnp.where(lane // 16 == row8, jnp.broadcast_to(final, (8, 128)), 0.0)
        lane_in = lax.broadcasted_iota(jnp.int32, (128, 128), 0)
        lane_out = lax.broadcasted_iota(jnp.int32, (128, 128), 1)
        pick = jnp.where(lane_in % 16 == lane_out, 1.0, 0.0)
        table_out[...] = jnp.dot(
            spread, pick, precision=lax.Precision.HIGHEST, preferred_element_type=jnp.float32
        )

    def sent():
        for ch in range(CHUNKS):
            for copy in step1_copies(ch, True):
                copy.wait_send()
            for dz in (1, 2, 3):
                (copyr if ch in EARLY_Z else copyz)(ch, dz).wait_send()
        for copy in quad_out(ecopy1) + quad_out(bcopy1):
            copy.wait_send()
        for n in (1, 2, 3):
            for small in (ecopy2, ecopy3, bcopy2, bcopy3):
                small(n).wait_send()

    loaded(0, 1)
    start1(0, slice(0, 4))
    for ch in range(2, CHUNKS):
        if ch not in EARLY_Z:
            load(ch)
    loaded(*EARLY_Z)
    startz(6)
    startz(7, (2,))
    segments1()
    for copy in fetches:
        copy.wait()
    start1(0, slice(4, 7))
    start1(1)
    clear()
    segments2()
    startz(7, (1, 3))
    first(0)
    segments3()
    start1(2)
    first(1)
    shares()
    start1(3)
    first(3)
    first(2)
    first(4)
    first(5)
    shares2()
    second(0)
    second(1)
    second(2)
    second(4)
    first(7)
    first(6)
    third(0)
    shares3()
    second(3)
    second(5)
    third(2)
    shares4()
    third(1)
    third(4)
    sent()
    third(3)
    third(7)
    third(6)
    third(5)

    for ch in range(CHUNKS):
        for q in (1, 2, 3):
            copyq(ch, q).wait_send()


def finish(hourly, table, out, depth):
    out[...] = hourly[...]
    depth[...] = (table[...] / table[:, HOURS : HOURS + 1])[:, :HOURS]


def body(reflectivity, scan_hour, basin_ids):
    def vmem(*shape):
        return pltpu.VMEM(shape, jnp.float32)

    def dma(*shape):
        return pltpu.SemaphoreType.DMA(shape)

    chunks = range(CHUNKS)
    scratch = [
        vmem(CHUNKS, 2, 2, 4, 4, 2, 8, 128),
        vmem(CHUNKS, 2, 2, 2, 4, 4, 8, 128),
        *[vmem(4, 1 if ch in EARLY_Z else SLOTS[ch % 2], 4, 8, 128) for ch in chunks],
        *[vmem(4, HOURS + LOW, *((8, 128) if ch in LATE_Z else (4, 8, 128))) for ch in chunks],
        *[vmem(4, SLOTS[1] if ch in LATE_Z else HOURS, 8, 128) for ch in chunks],
        *[vmem(3, *((SLOTS[1], 4) if ch in LATE_Z else (HOURS,)), 8, 128) for ch in chunks],
        vmem(2, 2, 2, 8, 128), vmem(2, 2, 2, 8, 128), vmem(4, HOURS // 4, 8, 128), vmem(3, HOURS // 4, 8, 128),
        vmem(HOURS // 4, 8, 128), vmem(3, HOURS // 4, 8, 128),
        vmem(8, 16, 128), vmem(8, 16, 128), vmem(16, 128), vmem(3, 16, 128), vmem(8, 128), vmem(3, 8, 128),
        dma(CHUNKS), dma(CHUNKS, 8), dma(CHUNKS, 8), dma(CHUNKS, 4), dma(CHUNKS, 4), dma(CHUNKS, 4), dma(CHUNKS, 4),
        dma(8), dma(8), dma(4), dma(4), dma(4), dma(4), dma(8), dma(8), dma(4), dma(4), dma(4), dma(4),
        *[vmem(4, 2, 2, 4, 2, 8, 128) for ch in EARLY_Z],
        dma(CHUNKS, 4), dma(CHUNKS, 4), dma(CHUNKS),
        pltpu.SMEM((128,), jnp.int32), pltpu.VMEM((2, 32), jnp.int32), dma(2),
    ]
    block = pl.BlockSpec(memory_space=pltpu.VMEM)
    hourly, table = pl.pallas_call(
        kernel,
        out_shape=(
            jax.ShapeDtypeStruct((HOURS, 32, 256), jnp.float32),
            jax.ShapeDtypeStruct((8, 128), jnp.float32),
        ),
        in_specs=[pl.BlockSpec(memory_space=pl.ANY)] * 3,
        out_specs=(block, block),
        scratch_shapes=scratch,
        compiler_params=pltpu.CompilerParams(
            collective_id=0, has_side_effects=True, vmem_limit_bytes=52 * 1024 * 1024
        ),
    )(reflectivity.reshape(4, 2, 2, BANDS, 8, 2048), scan_hour, basin_ids.T)
    return pl.pallas_call(
        finish,
        out_shape=(
            jax.ShapeDtypeStruct((HOURS, 32, 256), jnp.float32),
            jax.ShapeDtypeStruct((8, HOURS), jnp.float32),
        ),
        in_specs=[block, block],
        out_specs=(block, block),
        compiler_params=pltpu.CompilerParams(vmem_limit_bytes=8 * 1024 * 1024),
    )(hourly, table)


def solution(mesh):
    placed = (P(("row", "col"), None, None), P(), P("row", "col"))
    return jax.shard_map(
        body,
        mesh=mesh,
        in_specs=placed,
        out_specs=(P(None, "row", "col"), P(("row", "col"), None)),
        check_vma=False,
    )
```
